32 devices in a mesh: groups: 2 (over y), rows: 4 (over z), cols: 4 (over x, core).
Axes of the slice: x: 2, y: 2, z: 4, core: 2. Of those that a mesh axis runs over, the one named last changes fastest.
Arguments:
- tile_blocks: float32 [32, 32, 4, 128, 128], P(('groups', 'rows'), 'cols'), parts along dimension 0, may hold values from -1 to 3
- tile_codes: int32 [32, 32, 3], P(('groups', 'rows'), 'cols'), parts along dimension 0, may hold values from 0 to 3, as said below
- shifts: float32 [16], P('groups'), parts along dimension 0, may hold values from 1.2 to 2.8
- shift_order: int32 [16], P('groups'), parts along dimension 0, may hold values from 0 to 7, each once
- earlier: float32 [16, 32, 32, 128], P(None, ('groups', 'rows'), 'cols'), parts along dimension 1, may hold values from -60 to 60
- start_weights: float32 [32], P('groups'), parts along dimension 0, may hold values from -1 to 1
Outputs:
- new_basis: float32 [8, 32, 32, 128], P(None, ('groups', 'rows'), 'cols'), parts along dimension 1
- upper_factor: float32 [16, 8], P('groups'), parts along dimension 0
- projections: float32 [32, 8], P('groups'), parts along dimension 0
The draws below stay inside these ranges and needn't reach their ends.
There are 2 independent parts, one for each index of `groups`. The reference program is written for one: setup_inputs(seed, part) draws one part's arguments, and reference() takes and returns one part's arrays. A program takes and returns all parts, laid end to end along the dimension named above; each array names one. Nothing has to cross between parts.
Inputs may be any that keep to these rules, and one draw needn't show every extreme that they name: `tile_codes`: the three codes of one block are distinct. `shift_order`: each of 0 to 7 appears once.
All inputs are finite; a program needn't handle non-finite values.
Results may differ from the reference program's by a relative error of at most 0.0003.
Values sent between devices are 32-bit elements; how exact they have to be, the bound alone decides.
A program may use at most 64 MiB of HBM per device.

```python
import math
import jax
import jax.numpy as jnp
from jax import lax

TILE = 128
BASIS = 8
PREV = 16
NBR = 16
NBC = 32


def draw_tile_blocks(key, part):
    key_list = jax.random.split(jax.random.fold_in(key, 11), 2)
    shape_full = (NBR, NBC, 4, TILE, TILE)
    random_part = jnp.clip(jax.random.normal(key_list[0], shape_full, jnp.float32), -4.0, 4.0)
    spread = jax.random.uniform(key_list[1], (NBR, NBC, 4, 1, 1), jnp.float32, 0.7, 1.4)
    entries = 0.5 * random_part * spread / math.sqrt(TILE)
    identity = jnp.eye(TILE, dtype=jnp.float32)
    slot_mask = (jnp.arange(4) == 0).astype(jnp.float32)[:, None, None]
    return entries + 2.0 * slot_mask * identity


def draw_tile_codes(key, part):
    missing = jax.random.randint(jax.random.fold_in(key, 23), (NBR, NBC, 1), 0, 4, dtype=jnp.int32)
    offsets = jnp.arange(1, 4, dtype=jnp.int32)[None, None, :]
    return ((missing + offsets) % 4).astype(jnp.int32)


def draw_earlier(key, part):
    key_list = jax.random.split(jax.random.fold_in(key, 37), 2)
    shape_full = (PREV, NBR, NBC, TILE)
    random_part = jnp.clip(jax.random.normal(key_list[0], shape_full, jnp.float32), -4.0, 4.0)
    factor = jax.random.uniform(key_list[1], (1, NBR, NBC, 1), jnp.float32, 0.7, 1.4)
    row_level = jnp.arange(NBR, dtype=jnp.float32) / max(NBR - 1, 1)
    col_level = jnp.arange(NBC, dtype=jnp.float32) / max(NBC - 1, 1)
    profile = jnp.exp(math.log(3.0) * (row_level[:, None] + col_level[None, :]))
    raw = (random_part * factor * profile[None, :, :, None]).reshape(PREV, -1).T
    ortho, upper = jnp.linalg.qr(raw)
    total_cells = float(NBR * NBC * TILE)
    return (ortho.T * jnp.sqrt(total_cells)).reshape(shape_full).astype(jnp.float32)


def bell_draw(rng, dims, scale, most, held_as=jnp.bfloat16):
    array = jax.random.normal(rng, dims, jnp.float32) * scale
    return jnp.minimum(jnp.maximum(array, -most), most).astype(held_as)


def setup_inputs(seed: int = 0, part: int = 0) -> dict:
    seeds = jax.random.split(jax.random.key(seed), 7)
    part_splits = jax.random.split(jax.random.fold_in(seeds[6], part), 7)
    return {
        "tile_blocks": draw_tile_blocks(jax.random.fold_in(jax.random.fold_in(seeds[6], part), 71), part),
        "tile_codes": draw_tile_codes(jax.random.fold_in(jax.random.fold_in(seeds[6], part), 71), part),
        "shifts": jnp.clip(jax.random.uniform(part_splits[2], (BASIS,), jnp.float32, 1.2, 2.8), 1.2, 2.8),
        "shift_order": jax.random.permutation(part_splits[3], BASIS).astype(jnp.int32),
        "earlier": draw_earlier(jax.random.fold_in(jax.random.fold_in(seeds[6], part), 71), part),
        "start_weights": bell_draw(part_splits[5], (PREV,), 0.25, 1.0, jnp.float32),
    }


highest = lax.Precision.HIGHEST

def apply_operator(tile_blocks, tile_codes, vector):
    padded = jnp.pad(vector, ((1, 1), (1, 1), (0, 0)))
    beside = (padded[:-2, 1:-1], padded[2:, 1:-1], padded[1:-1, :-2], padded[1:-1, 2:])
    slots = [vector]
    for slot_index in range(3):
        code_column = tile_codes[:, :, slot_index]
        chosen = jnp.zeros_like(vector)
        for direction in range(4):
            chosen = chosen + jnp.where((code_column == direction)[:, :, None], beside[direction], jnp.zeros_like(vector))
        slots.append(chosen)
    stacked = jnp.stack(slots, axis=2)
    return jnp.einsum('rckij,rckj->rci', tile_blocks, stacked, precision=highest)

def reference(tile_blocks, tile_codes, shifts, shift_order, earlier, start_weights):
    picker = (shift_order[:, None] == jnp.arange(BASIS, dtype=jnp.int32)[None, :]).astype(shifts.dtype)
    shift_values = jnp.dot(picker, shifts, precision=highest)
    current = jnp.einsum('p,prct->rct', start_weights, earlier, precision=highest)
    columns = []
    for step_index in range(BASIS):
        current = apply_operator(tile_blocks, tile_codes, current) - shift_values[step_index] * current
        columns.append(current)
    powers = jnp.stack(columns)
    total_cells = float(NBR * NBC * TILE)
    projections = jnp.einsum('prct,srct->ps', earlier, powers, precision=highest) / total_cells
    cleaned = powers - jnp.einsum('ps,prct->srct', projections, earlier, precision=highest)
    flat = cleaned.reshape(BASIS, -1).T
    ortho, upper = jnp.linalg.qr(flat)
    signs = jnp.sign(jnp.diagonal(upper))
    upper_factor = upper * signs[:, None] / jnp.sqrt(total_cells)
    new_basis = (ortho * signs[None, :]).T.reshape(BASIS, NBR, NBC, TILE) * jnp.sqrt(total_cells)
    return (new_basis, upper_factor, projections)
```

```python
import functools

import jax
import jax.numpy as jnp
from jax import lax
from jax.experimental import pallas as pl
from jax.experimental.pallas import tpu as pltpu
from jax.sharding import PartitionSpec as P

MESH = pl.DeviceIdType.MESH
ABOVE, BELOW, LEFT, RIGHT = range(4)


def kernel(
    n_rows, n_cols, pitch,
    blocks_hbm, codes_hbm, shifts_hbm, order_hbm, earlier_hbm, weights_hbm,
    basis_ref, upper_ref, proj_ref,
    blocks, earlier, codes_ref, shifts_ref, order_ref, weights_ref,
    fields, chosen, halo_rows, halo_cols, edge_cols, rim_rows, rim_cols,
    code_table, stats, gathered, spread,
    load_sem, small_sem, send_sem, recv_sem, all_send, all_recv,
):
    rows, cols, slots, tile, _ = blocks.shape
    basis = basis_ref.shape[0]
    prev = earlier.shape[0]
    groups_prev = prev // basis
    peers = n_rows * n_cols
    cells = float(peers * rows * cols * tile)
    my_row, my_col = lax.axis_index("rows"), lax.axis_index("cols")
    me = my_row * n_cols + my_col

    def load(r, c):
        return pltpu.make_async_copy(
            blocks_hbm.at[r, c], blocks.at[r, c], load_sem.at[r, c]
        )

    small = [
        pltpu.make_async_copy(src, dst, small_sem.at[i])
        for i, (src, dst) in enumerate(
            [
                (weights_hbm, weights_ref),
                (earlier_hbm, earlier),
                (codes_hbm, codes_ref),
                (shifts_hbm, shifts_ref),
                (order_hbm, order_ref),
            ]
        )
    ]
    for copy in small:
        copy.start()
    for r in range(rows):
        for c in range(cols):
            load(r, c).start()

    barrier = pltpu.get_barrier_semaphore()

    def place(index):
        return {"rows": index // n_cols, "cols": index % n_cols}

    @pl.loop(1, peers)
    def _(d):
        pl.semaphore_signal(
            barrier, inc=1, device_id=place((me + d) % peers), device_id_type=MESH
        )

    for k in range(1, basis + 1):
        fields[k] = jnp.zeros((rows, cols, tile), jnp.float32)
    stats[...] = jnp.zeros_like(stats)
    no_row = jnp.zeros((basis, cols, tile), jnp.float32)
    no_col = jnp.zeros((basis, rows, tile), jnp.float32)
    has = [my_row > 0, my_row < n_rows - 1, my_col > 0, my_col < n_cols - 1]

    @pl.when(my_row == 0)
    def _():
        halo_rows[:, 0] = no_row

    @pl.when(my_row == n_rows - 1)
    def _():
        halo_rows[:, 1] = no_row

    @pl.when(my_col == 0)
    def _():
        halo_cols[:, 0] = no_col

    @pl.when(my_col == n_cols - 1)
    def _():
        halo_cols[:, 1] = no_col

    def hop(k, direction):
        if direction == ABOVE:
            src, dst, where_to = fields.at[k, 0], halo_rows.at[k, 1], {"rows": my_row - 1}
        elif direction == BELOW:
            src, dst, where_to = fields.at[k, rows - 1], halo_rows.at[k, 0], {"rows": my_row + 1}
        elif direction == LEFT:
            src, dst, where_to = edge_cols.at[k, 0], halo_cols.at[k, 1], {"cols": my_col - 1}
        else:
            src, dst, where_to = edge_cols.at[k, 1], halo_cols.at[k, 0], {"cols": my_col + 1}
        return pltpu.make_async_remote_copy(
            src_ref=src,
            dst_ref=dst,
            send_sem=send_sem.at[k, direction],
            recv_sem=recv_sem.at[k, direction ^ 1],
            device_id=where_to,
            device_id_type=MESH,
        )

    def arrival(k, direction):
        if direction in (ABOVE, BELOW):
            dst = halo_rows.at[k, direction]
        else:
            dst = halo_cols.at[k, direction - 2]
        return pltpu.make_async_copy(dst, dst, recv_sem.at[k, direction])

    def send(k, directions):
        for direction in directions:
            @pl.when(has[direction])
            def _(direction=direction):
                hop(k, direction).start()

    def receive(k):
        for direction in range(4):
            @pl.when(has[direction])
            def _(direction=direction):
                arrival(k, direction).wait()

    sublane = lax.broadcasted_iota(jnp.int32, (cols, tile), 0)
    lane = lax.broadcasted_iota(jnp.int32, (basis, tile), 1)
    diagonal = lax.broadcasted_iota(jnp.int32, (cols, cols), 0) == lax.broadcasted_iota(
        jnp.int32, (cols, cols), 1
    )

    def code_columns():
        codes = codes_ref[...].astype(jnp.float32)
        masks = []
        for s in range(slots - 1):
            masks.append([])
            for r in range(rows):
                line = jnp.broadcast_to(codes[s, r : r + 1], (cols, cols))
                column = jnp.sum(jnp.where(diagonal, line, 0.0), axis=1, keepdims=True)
                masks[s].append(jnp.broadcast_to(column, (cols, tile)))
        return masks

    def choose(k):
        none = jnp.zeros((cols, tile), jnp.float32)
        for r in range(rows):
            here = fields[k, r]
            above = fields[k, r - 1] if r > 0 else none
            below = fields[k, r + 1] if r < rows - 1 else none
            left = jnp.where(sublane == 0, 0.0, pltpu.roll(here, 1, 0))
            right = jnp.where(sublane == cols - 1, 0.0, pltpu.roll(here, cols - 1, 0))
            chosen[0, r] = here
            for s in range(slots - 1):
                code = code_table[s, r]
                chosen[s + 1, r] = jnp.where(
                    code < 1.5,
                    jnp.where(code < 0.5, above, below),
                    jnp.where(code < 2.5, left, right),
                )

    def inside(k, first):
        shift = shifts_ref[order_ref[k]]
        choose(k)

        @pl.loop(0, rows)
        def _(r):
            if first:
                for c in range(cols):
                    load(r, c).wait()
            for c in range(cols):
                total = blocks[r, c, 0] * chosen[0, r, c : c + 1]
                for s in range(1, slots):
                    total = total + blocks[r, c, s] * chosen[s, r, c : c + 1]
                product = jnp.sum(total.T, axis=0, keepdims=True)
                fields[k + 1, r, c : c + 1] = product - shift * chosen[0, r, c : c + 1]

    def pick(r, c, direction):
        total = jnp.zeros((tile, tile), jnp.float32)
        for s in range(slots - 1):
            code = code_table[s, r, c : c + 1]
            total = jnp.where(code == float(direction), blocks[r, c, s + 1], total)
        return total

    def gather_rim():
        for side in range(2):
            @pl.loop(0, cols)
            def _(c, side=side):
                total = jnp.zeros((tile, tile), jnp.float32)
                for s in range(slots - 1):
                    code = code_table[s, side * (rows - 1), pl.ds(c, 1)]
                    total = jnp.where(
                        code == float(side), blocks[side * (rows - 1), c, s + 1], total
                    )
                rim_rows[side, c] = total

            @pl.loop(0, rows)
            def _(r, side=side):
                rim_cols[side, r] = pick(r, side * (cols - 1), side + LEFT)

    def rim(k):
        for r in range(rows):
            for c in range(cols):
                parts = []
                for side in range(2):
                    if r == side * (rows - 1):
                        parts.append(rim_rows[side, c] * halo_rows[k, side, c : c + 1])
                    if c == side * (cols - 1):
                        parts.append(rim_cols[side, r] * halo_cols[k, side, r : r + 1])
                if parts:
                    product = jnp.sum(sum(parts[1:], parts[0]).T, axis=0, keepdims=True)
                    fields[k + 1, r, c : c + 1] += product

    def edges(k):
        for r in range(rows):
            edge_cols[k, 0, r : r + 1] = fields[k, r, 0:1]
            edge_cols[k, 1, r : r + 1] = fields[k, r, cols - 1 : cols]

    pairs = prev + basis
    per_line = tile // pitch
    pair_lane = lax.broadcasted_iota(jnp.int32, (pairs, tile), 1)
    pair_index = lax.broadcasted_iota(jnp.int32, (pairs, tile), 0)
    line_index = lax.broadcasted_iota(jnp.int32, stats.shape, 0)

    def inner(k):
        field = fields[k + 1]
        values = []
        for g in range(groups_prev + 1):
            if g < groups_prev:
                other = earlier[g * basis : (g + 1) * basis]
            else:
                other = fields[1 : basis + 1]
            values.append(jnp.sum(jnp.sum(other * field[None], axis=1), axis=1))
        value = jnp.sum(jnp.concatenate(values, axis=0), axis=1, keepdims=True)
        line = jnp.sum(
            jnp.where(pair_lane == (k % per_line) * pitch + pair_index, value, 0.0),
            axis=0,
            keepdims=True,
        )
        stats[...] += jnp.where(line_index == k // per_line, line, 0.0)

    small[0].wait()
    small[1].wait()
    start = weights_ref[0] * earlier[0]
    for p in range(1, prev):
        start = start + weights_ref[p] * earlier[p]
    fields[0] = start
    edges(0)
    for copy in small[2:]:
        copy.wait()
    for s, lines in enumerate(code_columns()):
        for r, line in enumerate(lines):
            code_table[s, r] = line
    pl.semaphore_wait(barrier, peers - 1)
    send(0, (ABOVE, BELOW, LEFT, RIGHT))
    inside(0, True)
    gather_rim()

    @pl.loop(0, basis - 1)
    def _(k):
        receive(k)
        rim(k)
        edges(k + 1)
        send(k + 1, (ABOVE, BELOW, LEFT, RIGHT))
        inside(k + 1, False)
        inner(k)

    receive(basis - 1)
    rim(basis - 1)
    inner(basis - 1)

    def deliver(d):
        return pltpu.make_async_remote_copy(
            src_ref=stats,
            dst_ref=gathered.at[me],
            send_sem=all_send.at[d],
            recv_sem=all_recv.at[me],
            device_id=place((me + d) % peers),
            device_id_type=MESH,
        )

    @pl.loop(1, peers)
    def _(d):
        deliver(d).start()

    gathered[me] = stats[...]

    @pl.loop(1, peers)
    def _(d):
        source = (me + d) % peers
        pltpu.make_async_copy(
            gathered.at[source], gathered.at[source], all_recv.at[source]
        ).wait()

    total = jnp.sum(gathered[...], axis=0) * (1.0 / cells)
    turned = total.T
    proj = [None] * pairs
    for k in range(basis):
        for g in range(groups_prev + 1):
            first = (k % per_line) * pitch + g * basis
            column = turned[first : first + basis, k // per_line : k // per_line + 1]
            column = jnp.broadcast_to(column, (basis, tile))
            spread[g * basis + k] = column
            proj[g * basis + k] = column
        first = (k % per_line) * pitch
        proj_ref[k : k + 1, :] = total[k // per_line : k // per_line + 1, first : first + prev]

    for k in range(basis):
        value = fields[k + 1]
        for p in range(prev):
            g, q = p // basis, p % basis
            value = value - spread[g * basis + k, q : q + 1][None] * earlier[p]
        basis_ref[k] = value

    gram = {}
    for j in range(basis):
        for k in range(j, basis):
            removed = proj[j] * proj[k]
            for g in range(1, groups_prev):
                removed = removed + proj[g * basis + j] * proj[g * basis + k]
            gram[j, k] = spread[groups_prev * basis + k, j : j + 1] - jnp.sum(
                removed, axis=0, keepdims=True
            )
    lower, inverse = {}, []
    for j in range(basis):
        root = jnp.sqrt(gram[j, j])
        inverse.append(1.0 / root)
        lower[j, j] = root
        for k in range(j + 1, basis):
            lower[k, j] = gram[j, k] * inverse[j]
        for k in range(j + 1, basis):
            for m in range(k, basis):
                gram[k, m] = gram[k, m] - lower[k, j] * lower[m, j]

    row_index = lax.broadcasted_iota(jnp.int32, (basis, tile), 0)
    upper = jnp.zeros((basis, tile), jnp.float32)
    for j in range(basis):
        line = jnp.zeros((1, tile), jnp.float32)
        for k in range(j, basis):
            line = jnp.where(lane[0:1] == k, lower[k, j], line)
        upper = jnp.where(row_index == j, line, upper)
    upper_ref[...] = upper[:, :basis]

    for r in range(rows):
        done = []
        for k in range(basis):
            value = basis_ref[k, r]
            for j in range(k):
                value = value - lower[k, j] * done[j]
            value = value * inverse[k]
            done.append(value)
            basis_ref[k, r] = value

    @pl.loop(0, basis)
    def _(k):
        for direction in range(4):
            @pl.when(has[direction])
            def _(direction=direction):
                hop(k, direction).wait_send()

    @pl.loop(1, peers)
    def _(d):
        deliver(d).wait_send()


def store(basis_ref, upper_ref, proj_ref, basis_hbm, upper_hbm, proj_hbm, sem):
    copies = [
        pltpu.make_async_copy(src, dst, sem.at[i])
        for i, (src, dst) in enumerate(
            [(basis_ref, basis_hbm), (upper_ref, upper_hbm), (proj_ref, proj_hbm)]
        )
    ]
    for copy in copies:
        copy.start()
    for copy in copies:
        copy.wait()


def shards(n_rows, n_cols, tile_blocks, tile_codes, shifts, shift_order, earlier, start_weights):
    rows, cols, slots, tile, _ = tile_blocks.shape
    basis, prev = shifts.shape[0], earlier.shape[0]
    peers = n_rows * n_cols
    pitch = pl.next_power_of_2(prev + basis)
    lines = pl.cdiv(basis, tile // pitch)
    vmem = pl.BlockSpec(memory_space=pltpu.VMEM)
    hbm = pl.BlockSpec(memory_space=pltpu.HBM)
    codes = jnp.transpose(tile_codes, (2, 0, 1))
    f32 = jnp.float32
    basis_out, upper, proj = pl.pallas_call(
        functools.partial(kernel, n_rows, n_cols, pitch),
        out_shape=(
            jax.ShapeDtypeStruct((basis, rows, cols, tile), f32),
            jax.ShapeDtypeStruct((basis, basis), f32),
            jax.ShapeDtypeStruct((basis, prev), f32),
        ),
        in_specs=[hbm] * 6,
        out_specs=(vmem, vmem, vmem),
        scratch_shapes=[
            pltpu.VMEM(tile_blocks.shape, f32),
            pltpu.VMEM(earlier.shape, f32),
            pltpu.VMEM(codes.shape, jnp.int32),
            pltpu.SMEM(shifts.shape, f32),
            pltpu.SMEM(shift_order.shape, jnp.int32),
            pltpu.SMEM(start_weights.shape, f32),
            pltpu.VMEM((basis + 1, rows, cols, tile), f32),
            pltpu.VMEM((slots, rows, cols, tile), f32),
            pltpu.VMEM((basis, 2, cols, tile), f32),
            pltpu.VMEM((basis, 2, rows, tile), f32),
            pltpu.VMEM((basis, 2, rows, tile), f32),
            pltpu.VMEM((2, cols, tile, tile), f32),
            pltpu.VMEM((2, rows, tile, tile), f32),
            pltpu.VMEM((slots - 1, rows, cols, tile), f32),
            pltpu.VMEM((lines, tile), f32),
            pltpu.VMEM((peers, lines, tile), f32),
            pltpu.VMEM(((prev // basis + 1) * basis, basis, tile), f32),
            pltpu.SemaphoreType.DMA((rows, cols)),
            pltpu.SemaphoreType.DMA((5,)),
            pltpu.SemaphoreType.DMA((basis, 4)),
            pltpu.SemaphoreType.DMA((basis, 4)),
            pltpu.SemaphoreType.DMA((peers,)),
            pltpu.SemaphoreType.DMA((peers,)),
        ],
        compiler_params=pltpu.CompilerParams(
            collective_id=0, has_side_effects=True, vmem_limit_bytes=48 * 1024 * 1024
        ),
        name="sstep",
    )(*[pltpu.with_memory_space_constraint(x, pltpu.HBM) for x in (tile_blocks, codes, shifts, shift_order, earlier, start_weights)])
    results = (basis_out, upper, proj)
    basis_out, upper, proj = pl.pallas_call(
        store,
        out_shape=tuple(jax.ShapeDtypeStruct(x.shape, f32) for x in results),
        in_specs=[vmem] * 3,
        out_specs=(hbm,) * 3,
        scratch_shapes=[pltpu.SemaphoreType.DMA((3,))],
        name="store",
    )(*[pltpu.with_memory_space_constraint(x, pltpu.VMEM) for x in results])
    return basis_out, upper, proj.T


def solution(mesh):
    in_specs = (
        P(("groups", "rows"), "cols", None, None, None),
        P(("groups", "rows"), "cols", None),
        P("groups"),
        P("groups"),
        P(None, ("groups", "rows"), "cols", None),
        P("groups"),
    )
    out_specs = (P(None, ("groups", "rows"), "cols", None), P("groups", None), P("groups", None))
    body = functools.partial(shards, mesh.shape["rows"], mesh.shape["cols"])
    return jax.shard_map(body, mesh=mesh, in_specs=in_specs, out_specs=out_specs, check_vma=False)
```

```python
import functools

import jax
import jax.numpy as jnp
from jax import lax
from jax.experimental import pallas as pl
from jax.experimental.pallas import tpu as pltpu
from jax.sharding import PartitionSpec as P

MESH = pl.DeviceIdType.MESH
ABOVE, BELOW, LEFT, RIGHT = range(4)


def kernel(
    n_rows, n_cols, pitch,
    blocks_hbm, codes_hbm, shifts_hbm, order_hbm, earlier_hbm, weights_hbm,
    basis_ref, upper_ref, proj_ref,
    blocks, earlier, codes_ref, shifts_ref, order_ref, weights_ref,
    fields, chosen, packed, rim_packed, halo_rows, halo_cols, edge_cols, rim_rows, rim_cols,
    code_table, stats, gathered, spread,
    load_sem, small_sem, send_sem, recv_sem, all_send, all_recv,
):
    rows, cols, slots, tile, _ = blocks.shape
    basis = basis_ref.shape[0]
    prev = earlier.shape[0]
    groups_prev = prev // basis
    peers = n_rows * n_cols
    cells = float(peers * rows * cols * tile)
    my_row, my_col = lax.axis_index("rows"), lax.axis_index("cols")
    me = my_row * n_cols + my_col

    def load(r, c):
        return pltpu.make_async_copy(
            blocks_hbm.at[r, c], blocks.at[r, c], load_sem.at[r, c]
        )

    small = [
        pltpu.make_async_copy(src, dst, small_sem.at[i])
        for i, (src, dst) in enumerate(
            [
                (weights_hbm, weights_ref),
                (earlier_hbm, earlier),
                (codes_hbm, codes_ref),
                (shifts_hbm, shifts_ref),
                (order_hbm, order_ref),
            ]
        )
    ]
    for copy in small:
        copy.start()
    for r in range(rows):
        for c in range(cols):
            load(r, c).start()

    barrier = pltpu.get_barrier_semaphore()

    def place(index):
        return {"rows": index // n_cols, "cols": index % n_cols}

    @pl.loop(1, peers)
    def _(d):
        pl.semaphore_signal(
            barrier, inc=1, device_id=place((me + d) % peers), device_id_type=MESH
        )

    for k in range(1, basis + 1):
        fields[k] = jnp.zeros((rows, cols, tile), jnp.float32)
    stats[...] = jnp.zeros_like(stats)
    no_row = jnp.zeros((basis, cols, tile), jnp.float32)
    no_col = jnp.zeros((basis, rows, tile), jnp.float32)
    has = [my_row > 0, my_row < n_rows - 1, my_col > 0, my_col < n_cols - 1]

    @pl.when(my_row == 0)
    def _():
        halo_rows[:, 0] = no_row

    @pl.when(my_row == n_rows - 1)
    def _():
        halo_rows[:, 1] = no_row

    @pl.when(my_col == 0)
    def _():
        halo_cols[:, 0] = no_col

    @pl.when(my_col == n_cols - 1)
    def _():
        halo_cols[:, 1] = no_col

    def hop(k, direction):
        if direction == ABOVE:
            src, dst, where_to = packed.at[k, 0], halo_rows.at[k, 1], {"rows": my_row - 1}
        elif direction == BELOW:
            src, dst, where_to = packed.at[k, 1], halo_rows.at[k, 0], {"rows": my_row + 1}
        elif direction == LEFT:
            src, dst, where_to = edge_cols.at[k, 0], halo_cols.at[k, 1], {"cols": my_col - 1}
        else:
            src, dst, where_to = edge_cols.at[k, 1], halo_cols.at[k, 0], {"cols": my_col + 1}
        return pltpu.make_async_remote_copy(
            src_ref=src,
            dst_ref=dst,
            send_sem=send_sem.at[k, direction],
            recv_sem=recv_sem.at[k, direction ^ 1],
            device_id=where_to,
            device_id_type=MESH,
        )

    def arrival(k, direction):
        if direction in (ABOVE, BELOW):
            dst = halo_rows.at[k, direction]
        else:
            dst = halo_cols.at[k, direction - 2]
        return pltpu.make_async_copy(dst, dst, recv_sem.at[k, direction])

    def send(k, directions):
        for direction in directions:
            @pl.when(has[direction])
            def _(direction=direction):
                hop(k, direction).start()

    def receive(k, directions):
        for direction in directions:
            @pl.when(has[direction])
            def _(direction=direction):
                arrival(k, direction).wait()

    sublane = lax.broadcasted_iota(jnp.int32, (cols, tile), 0)
    lane = lax.broadcasted_iota(jnp.int32, (basis, tile), 1)
    diagonal = lax.broadcasted_iota(jnp.int32, (cols, cols), 0) == lax.broadcasted_iota(
        jnp.int32, (cols, cols), 1
    )

    lane_index = lax.broadcasted_iota(jnp.int32, (cols, tile), 1)
    offset = lane_index % cols - sublane
    n_parts = tile // cols

    def code_columns():
        codes = codes_ref[...].astype(jnp.float32)
        masks = []
        for s in range(slots - 1):
            masks.append([])
            for r in range(rows):
                line = jnp.broadcast_to(codes[s, r : r + 1], (cols, cols))
                column = jnp.sum(jnp.where(diagonal, line, 0.0), axis=1, keepdims=True)
                masks[s].append(jnp.broadcast_to(column, (cols, tile)))
        return masks

    def choose(k):
        none = jnp.zeros((cols, tile), jnp.float32)
        for r in range(rows):
            here = fields[k, r]
            above = fields[k, r - 1] if r > 0 else none
            below = fields[k, r + 1] if r < rows - 1 else none
            left = jnp.where(sublane == 0, 0.0, pltpu.roll(here, 1, 0))
            right = jnp.where(sublane == cols - 1, 0.0, pltpu.roll(here, cols - 1, 0))
            chosen[0, r] = here
            for s in range(slots - 1):
                code = code_table[s, r]
                chosen[s + 1, r] = jnp.where(
                    code < 1.5,
                    jnp.where(code < 0.5, above, below),
                    jnp.where(code < 2.5, left, right),
                )

    def inside(k, first):
        shift = shifts_ref[order_ref[k]]
        choose(k)

        @pl.loop(0, rows)
        def _(r):
            if first:
                for c in range(cols):
                    load(r, c).wait()
            for c in range(cols):
                total = blocks[r, c, 0] * chosen[0, r, c : c + 1]
                for s in range(1, slots):
                    total = total + blocks[r, c, s] * chosen[s, r, c : c + 1]
                product = jnp.sum(total.T, axis=0, keepdims=True)
                fields[k + 1, r, c : c + 1] = product - shift * chosen[0, r, c : c + 1]

    def pick(r, c, direction):
        total = jnp.zeros((tile, tile), jnp.float32)
        for s in range(slots - 1):
            code = code_table[s, r, c : c + 1]
            total = jnp.where(code == float(direction), blocks[r, c, s + 1], total)
        return total

    def gather_rim():
        for side in range(2):
            @pl.loop(0, cols)
            def _(c, side=side):
                total = jnp.zeros((tile, tile), jnp.float32)
                for s in range(slots - 1):
                    code = code_table[s, side * (rows - 1), pl.ds(c, 1)]
                    total = jnp.where(
                        code == float(side), blocks[side * (rows - 1), c, s + 1], total
                    )
                rim_rows[side, c] = total

            @pl.loop(0, rows)
            def _(r, side=side):
                rim_cols[side, r] = pick(r, side * (cols - 1), side + LEFT)

    def rim(k, with_rows):
        for r in range(rows):
            for c in range(cols):
                parts = []
                for side in range(2):
                    if with_rows and r == side * (rows - 1):
                        parts.append(rim_rows[side, c] * halo_rows[k, side, c : c + 1])
                    if c == side * (cols - 1):
                        parts.append(rim_cols[side, r] * halo_cols[k, side, r : r + 1])
                if parts:
                    product = jnp.sum(sum(parts[1:], parts[0]).T, axis=0, keepdims=True)
                    fields[k + 1, r, c : c + 1] += product

    def repack(block):
        total = jnp.where(offset == 0, block, 0.0)
        for shift in range(1, cols):
            turned = pltpu.roll(block, cols - shift, 0)
            total = jnp.where(offset == shift, pltpu.roll(turned, shift, 1), total)
            total = jnp.where(
                offset == shift - cols, pltpu.roll(turned, tile + shift - cols, 1), total
            )
        return total

    def pack_rim():
        for side in range(2):
            @pl.loop(0, n_parts // 4)
            def _(step, side=side):
                for part in range(4):
                    index = step * 4 + part
                    line = [
                        rim_rows[side, c, pl.ds(index * cols, cols)] for c in range(cols)
                    ]
                    bit = 1
                    while bit < cols:
                        low = (lane_index & bit) == 0
                        for c in range(cols):
                            if c & bit == 0:
                                a, b = line[c], line[c | bit]
                                line[c] = jnp.where(low, a, pltpu.roll(b, bit, 1))
                                line[c | bit] = jnp.where(low, pltpu.roll(a, tile - bit, 1), b)
                        bit *= 2
                    for c in range(cols):
                        rim_packed[side, c, index] = line[c]

            @pl.loop(0, cols)
            def _(c, side=side):
                line = [rim_packed[side, c, part] for part in range(n_parts)]
                bit = 1
                while bit < n_parts:
                    high = ((lane_index // cols) & bit) != 0
                    line = [
                        jnp.where(high, line[(part + bit) % n_parts], line[part])
                        for part in range(n_parts)
                    ]
                    bit *= 2
                for part in range(n_parts):
                    rim_packed[side, c, part] = line[part]

    def rim_line(k, side, inner_part):
        rows_in = [halo_rows[k, side, c : c + 1] for c in range(cols)]
        sums = [inner_part]
        for part in range(n_parts):
            total = rim_packed[side, 0, part] * rows_in[0]
            for c in range(1, cols):
                total = total + rim_packed[side, c, part] * rows_in[c]
            sums.append(pltpu.roll(total, part * cols, 1) if part else total)
        while len(sums) > 1:
            sums = [sum(sums[i + 1 : i + 2], sums[i]) for i in range(0, len(sums), 2)]
        return sums[0]

    def finish(k, last):
        receive(k, (LEFT, RIGHT))
        rim(k, False)
        inner_parts = [repack(fields[k + 1, side * (rows - 1)]) for side in range(2)]
        for side in range(2):
            receive(k, (side,))
            packed[k + 1, side] = rim_line(k, side, inner_parts[side])
            if not last:
                send(k + 1, (side,))
        for side in range(2):
            fields[k + 1, side * (rows - 1)] = repack(packed[k + 1, side])
        if not last:
            edges(k + 1)
            send(k + 1, (LEFT, RIGHT))

    def edges(k):
        for r in range(rows):
            edge_cols[k, 0, r : r + 1] = fields[k, r, 0:1]
            edge_cols[k, 1, r : r + 1] = fields[k, r, cols - 1 : cols]

    pairs = prev + basis
    per_line = tile // pitch
    pair_lane = lax.broadcasted_iota(jnp.int32, (pairs, tile), 1)
    pair_index = lax.broadcasted_iota(jnp.int32, (pairs, tile), 0)
    line_index = lax.broadcasted_iota(jnp.int32, stats.shape, 0)

    def inner(k):
        field = fields[k + 1]
        values = []
        for g in range(groups_prev + 1):
            if g < groups_prev:
                other = earlier[g * basis : (g + 1) * basis]
            else:
                other = fields[1 : basis + 1]
            values.append(jnp.sum(jnp.sum(other * field[None], axis=1), axis=1))
        value = jnp.sum(jnp.concatenate(values, axis=0), axis=1, keepdims=True)
        line = jnp.sum(
            jnp.where(pair_lane == (k % per_line) * pitch + pair_index, value, 0.0),
            axis=0,
            keepdims=True,
        )
        stats[...] += jnp.where(line_index == k // per_line, line, 0.0)

    small[0].wait()
    small[1].wait()
    start = weights_ref[0] * earlier[0]
    for p in range(1, prev):
        start = start + weights_ref[p] * earlier[p]
    fields[0] = start
    for side in range(2):
        packed[0, side] = fields[0, side * (rows - 1)]
    edges(0)
    for copy in small[2:]:
        copy.wait()
    for s, lines in enumerate(code_columns()):
        for r, line in enumerate(lines):
            code_table[s, r] = line
    pl.semaphore_wait(barrier, peers - 1)
    send(0, (ABOVE, BELOW, LEFT, RIGHT))
    inside(0, True)
    gather_rim()

    receive(0, range(4))
    rim(0, True)
    for side in range(2):
        packed[1, side] = repack(fields[1, side * (rows - 1)])
    edges(1)
    send(1, range(4))
    inside(1, False)
    pack_rim()
    inner(0)

    @pl.loop(1, basis - 1)
    def _(k):
        finish(k, False)
        inside(k + 1, False)
        inner(k)

    finish(basis - 1, True)
    inner(basis - 1)

    def deliver(d):
        return pltpu.make_async_remote_copy(
            src_ref=stats,
            dst_ref=gathered.at[me],
            send_sem=all_send.at[d],
            recv_sem=all_recv.at[me],
            device_id=place((me + d) % peers),
            device_id_type=MESH,
        )

    @pl.loop(1, peers)
    def _(d):
        deliver(d).start()

    gathered[me] = stats[...]

    @pl.loop(1, peers)
    def _(d):
        source = (me + d) % peers
        pltpu.make_async_copy(
            gathered.at[source], gathered.at[source], all_recv.at[source]
        ).wait()

    total = jnp.sum(gathered[...], axis=0) * (1.0 / cells)
    turned = total.T
    proj = [None] * pairs
    for k in range(basis):
        for g in range(groups_prev + 1):
            first = (k % per_line) * pitch + g * basis
            column = turned[first : first + basis, k // per_line : k // per_line + 1]
            column = jnp.broadcast_to(column, (basis, tile))
            spread[g * basis + k] = column
            proj[g * basis + k] = column
        first = (k % per_line) * pitch
        proj_ref[k : k + 1, :] = total[k // per_line : k // per_line + 1, first : first + prev]

    for k in range(basis):
        value = fields[k + 1]
        for p in range(prev):
            g, q = p // basis, p % basis
            value = value - spread[g * basis + k, q : q + 1][None] * earlier[p]
        basis_ref[k] = value

    gram = {}
    for j in range(basis):
        for k in range(j, basis):
            removed = proj[j] * proj[k]
            for g in range(1, groups_prev):
                removed = removed + proj[g * basis + j] * proj[g * basis + k]
            gram[j, k] = spread[groups_prev * basis + k, j : j + 1] - jnp.sum(
                removed, axis=0, keepdims=True
            )
    lower, inverse = {}, []
    for j in range(basis):
        root = jnp.sqrt(gram[j, j])
        inverse.append(1.0 / root)
        lower[j, j] = root
        for k in range(j + 1, basis):
            lower[k, j] = gram[j, k] * inverse[j]
        for k in range(j + 1, basis):
            for m in range(k, basis):
                gram[k, m] = gram[k, m] - lower[k, j] * lower[m, j]

    row_index = lax.broadcasted_iota(jnp.int32, (basis, tile), 0)
    upper = jnp.zeros((basis, tile), jnp.float32)
    for j in range(basis):
        line = jnp.zeros((1, tile), jnp.float32)
        for k in range(j, basis):
            line = jnp.where(lane[0:1] == k, lower[k, j], line)
        upper = jnp.where(row_index == j, line, upper)
    upper_ref[...] = upper[:, :basis]

    for r in range(rows):
        done = []
        for k in range(basis):
            value = basis_ref[k, r]
            for j in range(k):
                value = value - lower[k, j] * done[j]
            value = value * inverse[k]
            done.append(value)
            basis_ref[k, r] = value

    @pl.loop(0, basis)
    def _(k):
        for direction in range(4):
            @pl.when(has[direction])
            def _(direction=direction):
                hop(k, direction).wait_send()

    @pl.loop(1, peers)
    def _(d):
        deliver(d).wait_send()


def store(basis_ref, upper_ref, proj_ref, basis_hbm, upper_hbm, proj_hbm, sem):
    copies = [
        pltpu.make_async_copy(src, dst, sem.at[i])
        for i, (src, dst) in enumerate(
            [(basis_ref, basis_hbm), (upper_ref, upper_hbm), (proj_ref, proj_hbm)]
        )
    ]
    for copy in copies:
        copy.start()
    for copy in copies:
        copy.wait()


def shards(n_rows, n_cols, tile_blocks, tile_codes, shifts, shift_order, earlier, start_weights):
    rows, cols, slots, tile, _ = tile_blocks.shape
    basis, prev = shifts.shape[0], earlier.shape[0]
    peers = n_rows * n_cols
    pitch = pl.next_power_of_2(prev + basis)
    lines = pl.cdiv(basis, tile // pitch)
    vmem = pl.BlockSpec(memory_space=pltpu.VMEM)
    hbm = pl.BlockSpec(memory_space=pltpu.HBM)
    codes = jnp.transpose(tile_codes, (2, 0, 1))
    f32 = jnp.float32
    basis_out, upper, proj = pl.pallas_call(
        functools.partial(kernel, n_rows, n_cols, pitch),
        out_shape=(
            jax.ShapeDtypeStruct((basis, rows, cols, tile), f32),
            jax.ShapeDtypeStruct((basis, basis), f32),
            jax.ShapeDtypeStruct((basis, prev), f32),
        ),
        in_specs=[hbm] * 6,
        out_specs=(vmem, vmem, vmem),
        scratch_shapes=[
            pltpu.VMEM(tile_blocks.shape, f32),
            pltpu.VMEM(earlier.shape, f32),
            pltpu.VMEM(codes.shape, jnp.int32),
            pltpu.SMEM(shifts.shape, f32),
            pltpu.SMEM(shift_order.shape, jnp.int32),
            pltpu.SMEM(start_weights.shape, f32),
            pltpu.VMEM((basis + 1, rows, cols, tile), f32),
            pltpu.VMEM((slots, rows, cols, tile), f32),
            pltpu.VMEM((basis + 1, 2, cols, tile), f32),
            pltpu.VMEM((2, cols, tile // cols, cols, tile), f32),
            pltpu.VMEM((basis, 2, cols, tile), f32),
            pltpu.VMEM((basis, 2, rows, tile), f32),
            pltpu.VMEM((basis, 2, rows, tile), f32),
            pltpu.VMEM((2, cols, tile, tile), f32),
            pltpu.VMEM((2, rows, tile, tile), f32),
            pltpu.VMEM((slots - 1, rows, cols, tile), f32),
            pltpu.VMEM((lines, tile), f32),
            pltpu.VMEM((peers, lines, tile), f32),
            pltpu.VMEM(((prev // basis + 1) * basis, basis, tile), f32),
            pltpu.SemaphoreType.DMA((rows, cols)),
            pltpu.SemaphoreType.DMA((5,)),
            pltpu.SemaphoreType.DMA((basis, 4)),
            pltpu.SemaphoreType.DMA((basis, 4)),
            pltpu.SemaphoreType.DMA((peers,)),
            pltpu.SemaphoreType.DMA((peers,)),
        ],
        compiler_params=pltpu.CompilerParams(
            collective_id=0, has_side_effects=True, vmem_limit_bytes=48 * 1024 * 1024
        ),
        name="sstep",
    )(*[pltpu.with_memory_space_constraint(x, pltpu.HBM) for x in (tile_blocks, codes, shifts, shift_order, earlier, start_weights)])
    results = (basis_out, upper, proj)
    basis_out, upper, proj = pl.pallas_call(
        store,
        out_shape=tuple(jax.ShapeDtypeStruct(x.shape, f32) for x in results),
        in_specs=[vmem] * 3,
        out_specs=(hbm,) * 3,
        scratch_shapes=[pltpu.SemaphoreType.DMA((3,))],
        name="store",
    )(*[pltpu.with_memory_space_constraint(x, pltpu.VMEM) for x in results])
    return basis_out, upper, proj.T


def solution(mesh):
    in_specs = (
        P(("groups", "rows"), "cols", None, None, None),
        P(("groups", "rows"), "cols", None),
        P("groups"),
        P("groups"),
        P(None, ("groups", "rows"), "cols", None),
        P("groups"),
    )
    out_specs = (P(None, ("groups", "rows"), "cols", None), P("groups", None), P("groups", None))
    body = functools.partial(shards, mesh.shape["rows"], mesh.shape["cols"])
    return jax.shard_map(body, mesh=mesh, in_specs=in_specs, out_specs=out_specs, check_vma=False)
```

```python
import functools

import jax
import jax.numpy as jnp
from jax import lax
from jax.experimental import pallas as pl
from jax.experimental.pallas import tpu as pltpu
from jax.sharding import PartitionSpec as P

MESH = pl.DeviceIdType.MESH
ABOVE, BELOW, LEFT, RIGHT = range(4)


def kernel(
    n_rows, n_cols, pitch,
    blocks_hbm, codes_hbm, shifts_hbm, order_hbm, earlier_hbm, weights_hbm,
    basis_ref, upper_ref, proj_ref,
    blocks, earlier, codes_ref, shifts_ref, order_ref, weights_ref,
    fields, chosen, packed, cross, rim_packed, halo_rows, halo_cols, first_cols, edge_cols, rim_tiles,
    code_table, stats, gathered, late, late_gathered, spread,
    load_sem, small_sem, send_sem, recv_sem, all_sem,
):
    rows, cols, slots, tile, _ = blocks.shape
    basis = basis_ref.shape[0]
    prev = earlier.shape[0]
    groups_prev = prev // basis
    peers = n_rows * n_cols
    cells = float(peers * rows * cols * tile)
    my_row, my_col = lax.axis_index("rows"), lax.axis_index("cols")
    me = my_row * n_cols + my_col

    barrier = pltpu.get_barrier_semaphore()
    all_rows = [lax.rem(my_row + d, n_rows) for d in range(n_rows)]
    all_cols = [lax.rem(my_col + d, n_cols) for d in range(n_cols)]
    others = [{"rows": r, "cols": c} for r in all_rows for c in all_cols][1:]
    for other in others:
        pl.semaphore_signal(barrier, inc=1, device_id=other, device_id_type=MESH)

    def load(r, c):
        return pltpu.make_async_copy(
            blocks_hbm.at[r, c], blocks.at[r, c], load_sem.at[r, c]
        )

    small = [
        pltpu.make_async_copy(src, dst, small_sem.at[i])
        for i, (src, dst) in enumerate(
            [
                (weights_hbm, weights_ref),
                (earlier_hbm, earlier),
                (codes_hbm, codes_ref),
                (shifts_hbm, shifts_ref),
                (order_hbm, order_ref),
            ]
        )
    ]
    for copy in small:
        copy.start()
    for r in range(rows):
        for c in range(cols):
            load(r, c).start()

    for k in range(1, basis + 1):
        fields[k] = jnp.zeros((rows, cols, tile), jnp.float32)
    stats[...] = jnp.zeros_like(stats)
    no_row = jnp.zeros((basis, cols, tile), jnp.float32)
    no_first = jnp.zeros((rows, tile), jnp.float32)
    has = [my_row > 0, my_row < n_rows - 1, my_col > 0, my_col < n_cols - 1]

    @pl.when(my_row == 0)
    def _():
        halo_rows[:, 0] = no_row

    @pl.when(my_row == n_rows - 1)
    def _():
        halo_rows[:, 1] = no_row

    @pl.when(my_col == 0)
    def _():
        halo_cols[:, 0] = no_row
        first_cols[0] = no_first

    @pl.when(my_col == n_cols - 1)
    def _():
        halo_cols[:, 1] = no_row
        first_cols[1] = no_first

    def hop(k, direction, first=False):
        if direction == ABOVE:
            src, dst, where_to = packed.at[k, 0], halo_rows.at[k, 1], {"rows": my_row - 1}
        elif direction == BELOW:
            src, dst, where_to = packed.at[k, rows - 1], halo_rows.at[k, 0], {"rows": my_row + 1}
        else:
            side = direction - LEFT
            where_to = {"cols": my_col + 2 * side - 1}
            if first:
                src, dst = edge_cols.at[side], first_cols.at[1 - side]
            else:
                src, dst = cross.at[k], halo_cols.at[k, 1 - side]
        return pltpu.make_async_remote_copy(
            src_ref=src,
            dst_ref=dst,
            send_sem=send_sem.at[k, direction],
            recv_sem=recv_sem.at[k, direction ^ 1],
            device_id=where_to,
            device_id_type=MESH,
        )

    def arrival(k, direction, first):
        if direction in (ABOVE, BELOW):
            dst = halo_rows.at[k, direction]
        elif first:
            dst = first_cols.at[direction - LEFT]
        else:
            dst = halo_cols.at[k, direction - LEFT]
        return pltpu.make_async_copy(dst, dst, recv_sem.at[k, direction])

    def send(k, directions, first=False):
        for direction in directions:
            @pl.when(has[direction])
            def _(direction=direction):
                hop(k, direction, first).start()

    def receive(k, directions, first=False):
        for direction in directions:
            @pl.when(has[direction])
            def _(direction=direction):
                arrival(k, direction, first).wait()

    sublane = lax.broadcasted_iota(jnp.int32, (cols, tile), 0)
    lane = lax.broadcasted_iota(jnp.int32, (basis, tile), 1)
    diagonal = lax.broadcasted_iota(jnp.int32, (cols, cols), 0) == lax.broadcasted_iota(
        jnp.int32, (cols, cols), 1
    )

    lane_index = lax.broadcasted_iota(jnp.int32, (cols, tile), 1)
    within = lane_index % cols
    offset = within - sublane
    n_parts = tile // cols

    def code_columns():
        codes = codes_ref[...].astype(jnp.float32)
        masks = []
        for s in range(slots - 1):
            masks.append([])
            for r in range(rows):
                line = jnp.broadcast_to(codes[s, r : r + 1], (cols, cols))
                column = jnp.sum(jnp.where(diagonal, line, 0.0), axis=1, keepdims=True)
                masks[s].append(jnp.broadcast_to(column, (cols, tile)))
        return masks

    def choose(k):
        none = jnp.zeros((cols, tile), jnp.float32)
        for r in range(rows):
            here = fields[k, r]
            above = fields[k, r - 1] if r > 0 else none
            below = fields[k, r + 1] if r < rows - 1 else none
            left = jnp.where(sublane == 0, 0.0, pltpu.roll(here, 1, 0))
            right = jnp.where(sublane == cols - 1, 0.0, pltpu.roll(here, cols - 1, 0))
            chosen[0, r] = here
            for s in range(slots - 1):
                code = code_table[s, r]
                chosen[s + 1, r] = jnp.where(
                    code < 1.5,
                    jnp.where(code < 0.5, above, below),
                    jnp.where(code < 2.5, left, right),
                )

    def inside(k, first):
        shift = shifts_ref[order_ref[k]]
        choose(k)

        @pl.loop(0, rows)
        def _(r):
            if first:
                for c in range(cols):
                    load(r, c).wait()
            for c in range(cols):
                total = blocks[r, c, 0] * chosen[0, r, c : c + 1]
                for s in range(1, slots):
                    total = total + blocks[r, c, s] * chosen[s, r, c : c + 1]
                product = jnp.sum(total.T, axis=0, keepdims=True)
                fields[k + 1, r, c : c + 1] = product - shift * chosen[0, r, c : c + 1]

    def pick(r, c, direction):
        total = jnp.zeros((tile, tile), jnp.float32)
        for s in range(slots - 1):
            code = code_table[s, r, c : c + 1]
            total = jnp.where(code == float(direction), blocks[r, c, s + 1], total)
        return total

    def gather_rim():
        for side in range(2):
            @pl.loop(0, cols)
            def _(c, side=side):
                total = jnp.zeros((tile, tile), jnp.float32)
                for s in range(slots - 1):
                    code = code_table[s, side * (rows - 1), pl.ds(c, 1)]
                    total = jnp.where(
                        code == float(side), blocks[side * (rows - 1), c, s + 1], total
                    )
                rim_tiles[side, c] = total

            @pl.loop(0, rows)
            def _(r, side=side):
                rim_tiles[2, side * rows + r] = pick(r, side * (cols - 1), side + LEFT)

    def rim():
        for r in range(rows):
            for c in range(cols):
                parts = []
                for side in range(2):
                    if r == side * (rows - 1):
                        parts.append(rim_tiles[side, c] * halo_rows[0, side, c : c + 1])
                    if c == side * (cols - 1):
                        parts.append(
                            rim_tiles[2, side * rows + r] * first_cols[side, r : r + 1]
                        )
                if parts:
                    product = jnp.sum(sum(parts[1:], parts[0]).T, axis=0, keepdims=True)
                    fields[1, r, c : c + 1] += product

    def repack(block):
        total = jnp.where(offset == 0, block, 0.0)
        for shift in range(1, cols):
            turned = pltpu.roll(block, cols - shift, 0)
            total = jnp.where(offset == shift, pltpu.roll(turned, shift, 1), total)
            total = jnp.where(
                offset == shift - cols, pltpu.roll(turned, tile + shift - cols, 1), total
            )
        return total

    def pack_rim():
        @pl.loop(0, 3)
        def _(group):
            bit = 1
            while bit < cols:
                low = (lane_index & bit) == 0
                for part in range(n_parts):
                    for c in range(cols):
                        if c & bit == 0:
                            if bit == 1:
                                a, b = (
                                    rim_tiles[group, i, part * cols : (part + 1) * cols]
                                    for i in (c, c | bit)
                                )
                            else:
                                a, b = (rim_packed[group, i, part] for i in (c, c | bit))
                            rim_packed[group, c, part] = jnp.where(low, a, pltpu.roll(b, bit, 1))
                            rim_packed[group, c | bit, part] = jnp.where(
                                low, pltpu.roll(a, tile - bit, 1), b
                            )
                bit *= 2

            @pl.loop(0, cols)
            def _(c):
                line = [rim_packed[group, c, part] for part in range(n_parts)]
                bit = 1
                while bit < n_parts:
                    high = ((lane_index // cols) & bit) != 0
                    line = [
                        jnp.where(high, line[(part + bit) % n_parts], line[part])
                        for part in range(n_parts)
                    ]
                    bit *= 2
                for part in range(n_parts):
                    rim_packed[group, c, part] = line[part]

    def turn(block, shift):
        return pltpu.roll(block, shift % tile, 1) if shift % tile else block

    def rim_line(group, rows_in, sums):
        for part in range(n_parts):
            total = rim_packed[group, 0, part] * rows_in[0]
            for c in range(1, cols):
                total = total + rim_packed[group, c, part] * rows_in[c]
            sums = sums + [turn(total, part * cols)]
        while len(sums) > 1:
            sums = [sum(sums[i + 1 : i + 2], sums[i]) for i in range(0, len(sums), 2)]
        return sums[0]

    def crossing(lines, total):
        for r, block in lines:
            total = jnp.where(within == rows + r, turn(block, rows + r), total)
            total = jnp.where(within == r, turn(block, r + 1 - cols), total)
        return total

    middle = range(1, rows - 1)
    outer = [0, rows - 1]
    nothing = jnp.zeros((cols, tile), jnp.float32)

    def finish(k, last):
        parts = [repack(fields[k + 1, r]) for r in range(rows)]
        receive(k, (LEFT, RIGHT))
        line = rim_line(
            2,
            [
                jnp.where(within < rows, halo_cols[k, 0, c : c + 1], halo_cols[k, 1, c : c + 1])
                for c in range(cols)
            ],
            [],
        )
        for r in range(rows):
            parts[r] = parts[r] + jnp.where(
                within == 0,
                turn(line, -r),
                jnp.where(within == cols - 1, turn(line, cols - 1 - rows - r), 0.0),
            )
        for r in middle:
            fields[k + 1, r] = repack(parts[r])
        if last:
            known = products(k, middle)
        else:
            known = crossing([(r, parts[r]) for r in middle], nothing)
        receive(k, (ABOVE, BELOW))
        for side, r in enumerate(outer):
            parts[r] = rim_line(
                side, [halo_rows[k, side, c : c + 1] for c in range(cols)], [parts[r]]
            )
            if not last:
                packed[k + 1, r] = parts[r]
        if not last:
            send(k + 1, (ABOVE, BELOW))
            cross[k + 1] = crossing([(r, parts[r]) for r in outer], known)
            send(k + 1, (LEFT, RIGHT))
        for r in outer:
            fields[k + 1, r] = repack(parts[r])
        if last:
            late[...] = line_of(known + products(k, outer), 0)

    def edges():
        for r in range(rows):
            edge_cols[0, r : r + 1] = fields[0, r, 0:1]
            edge_cols[1, r : r + 1] = fields[0, r, cols - 1 : cols]

    pairs = prev + basis
    per_line = tile // pitch
    pair_lane = lax.broadcasted_iota(jnp.int32, (pairs, tile), 1)
    pair_index = lax.broadcasted_iota(jnp.int32, (pairs, tile), 0)
    line_index = lax.broadcasted_iota(jnp.int32, stats.shape, 0)

    def products(k, lines):
        values = []
        for g in range(groups_prev + 1):
            total = None
            for r in lines:
                if g < groups_prev:
                    other = earlier[g * basis : (g + 1) * basis, r]
                else:
                    other = fields[1 : basis + 1, r]
                term = other * fields[k + 1, r][None]
                total = term if total is None else total + term
            values.append(jnp.sum(total, axis=1))
        return jnp.concatenate(values, axis=0)

    def inner(k):
        record(k, products(k, range(rows)))

    def line_of(values, start):
        value = jnp.sum(values, axis=1, keepdims=True)
        return jnp.sum(
            jnp.where(pair_lane == start + pair_index, value, 0.0), axis=0, keepdims=True
        )

    def record(k, values):
        line = line_of(values, (k % per_line) * pitch)
        stats[...] += jnp.where(line_index == k // per_line, line, 0.0)

    small[0].wait()
    small[1].wait()
    start = weights_ref[0] * earlier[0]
    for p in range(1, prev):
        start = start + weights_ref[p] * earlier[p]
    fields[0] = start
    for r in (0, rows - 1):
        packed[0, r] = fields[0, r]
    edges()
    pl.semaphore_wait(barrier, peers - 1)
    send(0, range(4), True)
    for copy in small[2:]:
        copy.wait()
    for s, lines in enumerate(code_columns()):
        for r, line in enumerate(lines):
            code_table[s, r] = line
    inside(0, True)
    gather_rim()

    receive(0, range(4), True)
    rim()
    lines = [(r, repack(fields[1, r])) for r in range(rows)]
    for r in (0, rows - 1):
        packed[1, r] = lines[r][1]
    send(1, (ABOVE, BELOW))
    cross[1] = crossing(lines, nothing)
    send(1, (LEFT, RIGHT))
    inside(1, False)
    pack_rim()

    @pl.loop(1, basis - 1)
    def _(k):
        finish(k, False)
        inside(k + 1, False)

        @pl.when(k == 1)
        def _():
            inner(0)

        inner(k)

    def deliver(src, dst, send_sem, recv_sem):
        for other in others:
            pltpu.make_async_remote_copy(
                src_ref=src,
                dst_ref=dst.at[me],
                send_sem=send_sem,
                recv_sem=recv_sem,
                device_id=other,
                device_id_type=MESH,
            ).start()

    def collect(dst, sem):
        whole = dst.at[pl.ds(0, peers - 1)]
        pltpu.make_async_copy(whole, whole, sem).wait()

    deliver(stats, gathered, all_sem.at[0], all_sem.at[1])
    gathered[me] = stats[...]
    finish(basis - 1, True)

    deliver(late, late_gathered, all_sem.at[2], all_sem.at[3])

    def sent(k, first):
        for direction in range(4):
            @pl.when(has[direction])
            def _(direction=direction):
                hop(k, direction, first).wait_send()

    sent(0, True)

    @pl.loop(1, basis)
    def _(k):
        sent(k, False)

    late_gathered[me] = late[...]
    collect(gathered, all_sem.at[0])
    collect(gathered, all_sem.at[1])
    newest = basis - 1
    total = jnp.sum(gathered[...], axis=0) * (1.0 / cells)
    turned = total.T
    proj = [None] * pairs
    for k in range(newest):
        for g in range(groups_prev + 1):
            first = (k % per_line) * pitch + g * basis
            column = turned[first : first + basis, k // per_line : k // per_line + 1]
            column = jnp.broadcast_to(column, (basis, tile))
            spread[g * basis + k] = column
            proj[g * basis + k] = column
        first = (k % per_line) * pitch
        proj_ref[k : k + 1, :] = total[k // per_line : k // per_line + 1, first : first + prev]

    def clean(k):
        value = fields[k + 1]
        for p in range(prev):
            g, q = p // basis, p % basis
            value = value - spread[g * basis + k, q : q + 1][None] * earlier[p]
        return value

    def gram_of(j, k):
        removed = proj[j] * proj[k]
        for g in range(1, groups_prev):
            removed = removed + proj[g * basis + j] * proj[g * basis + k]
        return spread[groups_prev * basis + k, j : j + 1] - jnp.sum(
            removed, axis=0, keepdims=True
        )

    for k in range(newest):
        basis_ref[k] = clean(k)
    gram = {(j, k): gram_of(j, k) for j in range(newest) for k in range(j, newest)}
    lower, inverse = {}, []
    for j in range(newest):
        root = jnp.sqrt(gram[j, j])
        inverse.append(1.0 / root)
        lower[j, j] = root
        for k in range(j + 1, newest):
            lower[k, j] = gram[j, k] * inverse[j]
        for k in range(j + 1, newest):
            for m in range(k, newest):
                gram[k, m] = gram[k, m] - lower[k, j] * lower[m, j]

    for r in range(rows):
        done = []
        for k in range(newest):
            value = basis_ref[k, r]
            for j in range(k):
                value = value - lower[k, j] * done[j]
            value = value * inverse[k]
            done.append(value)
            basis_ref[k, r] = value

    collect(late_gathered, all_sem.at[2])
    collect(late_gathered, all_sem.at[3])
    last_line = jnp.sum(late_gathered[...], axis=0) * (1.0 / cells)
    turned = jnp.broadcast_to(last_line, (tile, tile)).T
    for g in range(groups_prev + 1):
        column = turned[g * basis : (g + 1) * basis]
        spread[g * basis + newest] = column
        proj[g * basis + newest] = column
    proj_ref[newest : newest + 1, :] = last_line[:, :prev]
    square = gram_of(newest, newest)
    for j in range(newest):
        value = gram_of(j, newest)
        for i in range(j):
            value = value - lower[j, i] * lower[newest, i]
        lower[newest, j] = value * inverse[j]
        square = square - lower[newest, j] * lower[newest, j]
    lower[newest, newest] = jnp.sqrt(square)
    value = clean(newest)
    for j in range(newest):
        value = value - lower[newest, j][None] * basis_ref[j]
    basis_ref[newest] = value * (1.0 / lower[newest, newest])[None]

    row_index = lax.broadcasted_iota(jnp.int32, (basis, tile), 0)
    upper = jnp.zeros((basis, tile), jnp.float32)
    for j in range(basis):
        line = jnp.zeros((1, tile), jnp.float32)
        for k in range(j, basis):
            line = jnp.where(lane[0:1] == k, lower[k, j], line)
        upper = jnp.where(row_index == j, line, upper)
    upper_ref[...] = upper[:, :basis]


def store(basis_ref, upper_ref, proj_ref, basis_hbm, upper_hbm, proj_hbm, sem):
    copies = [
        pltpu.make_async_copy(src, dst, sem.at[i])
        for i, (src, dst) in enumerate(
            [(basis_ref, basis_hbm), (upper_ref, upper_hbm), (proj_ref, proj_hbm)]
        )
    ]
    for copy in copies:
        copy.start()
    for copy in copies:
        copy.wait()


def shards(n_rows, n_cols, tile_blocks, tile_codes, shifts, shift_order, earlier, start_weights):
    rows, cols, slots, tile, _ = tile_blocks.shape
    basis, prev = shifts.shape[0], earlier.shape[0]
    peers = n_rows * n_cols
    pitch = pl.next_power_of_2(prev + basis)
    lines = pl.cdiv(basis, tile // pitch)
    vmem = pl.BlockSpec(memory_space=pltpu.VMEM)
    hbm = pl.BlockSpec(memory_space=pltpu.HBM)
    codes = jnp.transpose(tile_codes, (2, 0, 1))
    f32 = jnp.float32
    basis_out, upper, proj = pl.pallas_call(
        functools.partial(kernel, n_rows, n_cols, pitch),
        out_shape=(
            jax.ShapeDtypeStruct((basis, rows, cols, tile), f32),
            jax.ShapeDtypeStruct((basis, basis), f32),
            jax.ShapeDtypeStruct((basis, prev), f32),
        ),
        in_specs=[hbm] * 6,
        out_specs=(vmem, vmem, vmem),
        scratch_shapes=[
            pltpu.VMEM(tile_blocks.shape, f32),
            pltpu.VMEM(earlier.shape, f32),
            pltpu.VMEM(codes.shape, jnp.int32),
            pltpu.SMEM(shifts.shape, f32),
            pltpu.SMEM(shift_order.shape, jnp.int32),
            pltpu.SMEM(start_weights.shape, f32),
            pltpu.VMEM((basis + 1, rows, cols, tile), f32),
            pltpu.VMEM((slots, rows, cols, tile), f32),
            pltpu.VMEM((basis, rows, cols, tile), f32),
            pltpu.VMEM((basis, cols, tile), f32),
            pltpu.VMEM((3, cols, tile // cols, cols, tile), f32),
            pltpu.VMEM((basis, 2, cols, tile), f32),
            pltpu.VMEM((basis, 2, cols, tile), f32),
            pltpu.VMEM((2, rows, tile), f32),
            pltpu.VMEM((2, rows, tile), f32),
            pltpu.VMEM((3, cols, tile, tile), f32),
            pltpu.VMEM((slots - 1, rows, cols, tile), f32),
            pltpu.VMEM((lines, tile), f32),
            pltpu.VMEM((peers, lines, tile), f32),
            pltpu.VMEM((1, tile), f32),
            pltpu.VMEM((peers, 1, tile), f32),
            pltpu.VMEM(((prev // basis + 1) * basis, basis, tile), f32),
            pltpu.SemaphoreType.DMA((rows, cols)),
            pltpu.SemaphoreType.DMA((5,)),
            pltpu.SemaphoreType.DMA((basis, 4)),
            pltpu.SemaphoreType.DMA((basis, 4)),
            pltpu.SemaphoreType.DMA((4,)),
        ],
        compiler_params=pltpu.CompilerParams(
            collective_id=0, has_side_effects=True, vmem_limit_bytes=48 * 1024 * 1024
        ),
        name="sstep",
    )(*[pltpu.with_memory_space_constraint(x, pltpu.HBM) for x in (tile_blocks, codes, shifts, shift_order, earlier, start_weights)])
    results = (basis_out, upper, proj)
    basis_out, upper, proj = pl.pallas_call(
        store,
        out_shape=tuple(jax.ShapeDtypeStruct(x.shape, f32) for x in results),
        in_specs=[vmem] * 3,
        out_specs=(hbm,) * 3,
        scratch_shapes=[pltpu.SemaphoreType.DMA((3,))],
        name="store",
    )(*[pltpu.with_memory_space_constraint(x, pltpu.VMEM) for x in results])
    return basis_out, upper, proj.T


def solution(mesh):
    in_specs = (
        P(("groups", "rows"), "cols", None, None, None),
        P(("groups", "rows"), "cols", None),
        P("groups"),
        P("groups"),
        P(None, ("groups", "rows"), "cols", None),
        P("groups"),
    )
    out_specs = (P(None, ("groups", "rows"), "cols", None), P("groups", None), P("groups", None))
    body = functools.partial(shards, mesh.shape["rows"], mesh.shape["cols"])
    return jax.shard_map(body, mesh=mesh, in_specs=in_specs, out_specs=out_specs, check_vma=False)
```

```python
import functools

import jax
import jax.numpy as jnp
from jax import lax
from jax.experimental import pallas as pl
from jax.experimental.pallas import tpu as pltpu
from jax.sharding import PartitionSpec as P

MESH = pl.DeviceIdType.MESH
ABOVE, BELOW, LEFT, RIGHT = range(4)


def kernel(
    n_rows, n_cols, pitch,
    blocks_hbm, codes_hbm, shifts_hbm, order_hbm, earlier_hbm, weights_hbm,
    basis_ref, upper_ref, proj_ref,
    blocks, earlier, codes_ref, shifts_ref, order_ref, weights_ref,
    fields, chosen, packed, cross, rim_packed, halo_rows, halo_cols, first_cols, edge_cols, rim_tiles,
    code_table, stats, gathered, late, late_gathered, spread,
    load_sem, small_sem, send_sem, recv_sem, all_sem,
):
    rows, cols, slots, tile, _ = blocks.shape
    basis = basis_ref.shape[0]
    prev = earlier.shape[0]
    groups_prev = prev // basis
    peers = n_rows * n_cols
    cells = float(peers * rows * cols * tile)
    my_row, my_col = lax.axis_index("rows"), lax.axis_index("cols")
    me = my_row * n_cols + my_col

    barrier = pltpu.get_barrier_semaphore()
    all_rows = [lax.rem(my_row + d, n_rows) for d in range(n_rows)]
    all_cols = [lax.rem(my_col + d, n_cols) for d in range(n_cols)]
    others = [{"rows": r, "cols": c} for r in all_rows for c in all_cols][1:]
    others = others[n_cols - 1 :] + others[: n_cols - 1]
    for other in others:
        pl.semaphore_signal(barrier, inc=1, device_id=other, device_id_type=MESH)

    def load(r, c):
        return pltpu.make_async_copy(
            blocks_hbm.at[r, c], blocks.at[r, c], load_sem.at[r, c]
        )

    small = [
        pltpu.make_async_copy(src, dst, small_sem.at[i])
        for i, (src, dst) in enumerate(
            [
                (weights_hbm, weights_ref),
                (earlier_hbm, earlier),
                (codes_hbm, codes_ref),
                (shifts_hbm, shifts_ref),
                (order_hbm, order_ref),
            ]
        )
    ]
    for copy in small:
        copy.start()
    for r in range(0, 1):
        for c in range(cols):
            load(r, c).start()

    for k in range(1, basis + 1):
        fields[k] = jnp.zeros((rows, cols, tile), jnp.float32)
    stats[...] = jnp.zeros_like(stats)
    no_row = jnp.zeros((basis, cols, tile), jnp.float32)
    no_first = jnp.zeros((rows, tile), jnp.float32)
    has = [my_row > 0, my_row < n_rows - 1, my_col > 0, my_col < n_cols - 1]

    @pl.when(my_row == 0)
    def _():
        halo_rows[:, 0] = no_row

    @pl.when(my_row == n_rows - 1)
    def _():
        halo_rows[:, 1] = no_row

    @pl.when(my_col == 0)
    def _():
        halo_cols[:, 0] = no_row
        first_cols[0] = no_first

    @pl.when(my_col == n_cols - 1)
    def _():
        halo_cols[:, 1] = no_row
        first_cols[1] = no_first

    def hop(k, direction, first=False):
        if direction == ABOVE:
            src, dst, where_to = packed.at[k, 0], halo_rows.at[k, 1], {"rows": my_row - 1}
        elif direction == BELOW:
            src, dst, where_to = packed.at[k, rows - 1], halo_rows.at[k, 0], {"rows": my_row + 1}
        else:
            side = direction - LEFT
            where_to = {"cols": my_col + 2 * side - 1}
            if first:
                src, dst = edge_cols.at[side], first_cols.at[1 - side]
            else:
                src, dst = cross.at[k], halo_cols.at[k, 1 - side]
        return pltpu.make_async_remote_copy(
            src_ref=src,
            dst_ref=dst,
            send_sem=send_sem.at[k, direction],
            recv_sem=recv_sem.at[k, direction ^ 1],
            device_id=where_to,
            device_id_type=MESH,
        )

    def arrival(k, direction, first):
        if direction in (ABOVE, BELOW):
            dst = halo_rows.at[k, direction]
        elif first:
            dst = first_cols.at[direction - LEFT]
        else:
            dst = halo_cols.at[k, direction - LEFT]
        return pltpu.make_async_copy(dst, dst, recv_sem.at[k, direction])

    def send(k, directions, first=False):
        for direction in directions:
            @pl.when(has[direction])
            def _(direction=direction):
                hop(k, direction, first).start()

    def receive(k, directions, first=False):
        for direction in directions:
            @pl.when(has[direction])
            def _(direction=direction):
                arrival(k, direction, first).wait()

    sublane = lax.broadcasted_iota(jnp.int32, (cols, tile), 0)
    lane = lax.broadcasted_iota(jnp.int32, (basis, tile), 1)
    diagonal = lax.broadcasted_iota(jnp.int32, (cols, cols), 0) == lax.broadcasted_iota(
        jnp.int32, (cols, cols), 1
    )

    lane_index = lax.broadcasted_iota(jnp.int32, (cols, tile), 1)
    within = lane_index % cols
    offset = within - sublane
    n_parts = tile // cols

    def code_columns():
        codes = codes_ref[...].astype(jnp.float32)
        masks = []
        for s in range(slots - 1):
            masks.append([])
            for r in range(rows):
                line = jnp.broadcast_to(codes[s, r : r + 1], (cols, cols))
                column = jnp.sum(jnp.where(diagonal, line, 0.0), axis=1, keepdims=True)
                masks[s].append(jnp.broadcast_to(column, (cols, tile)))
        return masks

    def choose(k):
        none = jnp.zeros((cols, tile), jnp.float32)
        for r in range(rows):
            here = fields[k, r]
            above = fields[k, r - 1] if r > 0 else none
            below = fields[k, r + 1] if r < rows - 1 else none
            left = jnp.where(sublane == 0, 0.0, pltpu.roll(here, 1, 0))
            right = jnp.where(sublane == cols - 1, 0.0, pltpu.roll(here, cols - 1, 0))
            chosen[0, r] = here
            for s in range(slots - 1):
                code = code_table[s, r]
                chosen[s + 1, r] = jnp.where(
                    code < 1.5,
                    jnp.where(code < 0.5, above, below),
                    jnp.where(code < 2.5, left, right),
                )

    def inside(k, first):
        shift = shifts_ref[order_ref[k]]
        choose(k)

        @pl.loop(0, rows)
        def _(r):
            if first:
                for c in range(cols):
                    load(r, c).wait()
            for c in range(cols):
                total = blocks[r, c, 0] * chosen[0, r, c : c + 1]
                for s in range(1, slots):
                    total = total + blocks[r, c, s] * chosen[s, r, c : c + 1]
                product = jnp.sum(total.T, axis=0, keepdims=True)
                fields[k + 1, r, c : c + 1] = product - shift * chosen[0, r, c : c + 1]

    def pick(r, c, direction):
        total = jnp.zeros((tile, tile), jnp.float32)
        for s in range(slots - 1):
            code = code_table[s, r, c : c + 1]
            total = jnp.where(code == float(direction), blocks[r, c, s + 1], total)
        return total

    def gather_rim():
        for side in range(2):
            @pl.loop(0, cols)
            def _(c, side=side):
                total = jnp.zeros((tile, tile), jnp.float32)
                for s in range(slots - 1):
                    code = code_table[s, side * (rows - 1), pl.ds(c, 1)]
                    total = jnp.where(
                        code == float(side), blocks[side * (rows - 1), c, s + 1], total
                    )
                rim_tiles[side, c] = total

            @pl.loop(0, rows)
            def _(r, side=side):
                rim_tiles[2, side * rows + r] = pick(r, side * (cols - 1), side + LEFT)

    def rim():
        for r in range(rows):
            for c in range(cols):
                parts = []
                for side in range(2):
                    if r == side * (rows - 1):
                        parts.append(rim_tiles[side, c] * halo_rows[0, side, c : c + 1])
                    if c == side * (cols - 1):
                        parts.append(
                            rim_tiles[2, side * rows + r] * first_cols[side, r : r + 1]
                        )
                if parts:
                    product = jnp.sum(sum(parts[1:], parts[0]).T, axis=0, keepdims=True)
                    fields[1, r, c : c + 1] += product

    def repack(block):
        total = jnp.where(offset == 0, block, 0.0)
        for shift in range(1, cols):
            turned = pltpu.roll(block, cols - shift, 0)
            total = jnp.where(offset == shift, pltpu.roll(turned, shift, 1), total)
            total = jnp.where(
                offset == shift - cols, pltpu.roll(turned, tile + shift - cols, 1), total
            )
        return total

    def pack_rim():
        @pl.loop(0, 3)
        def _(group):
            bit = 1
            while bit < cols:
                low = (lane_index & bit) == 0
                for part in range(n_parts):
                    for c in range(cols):
                        if c & bit == 0:
                            if bit == 1:
                                a, b = (
                                    rim_tiles[group, i, part * cols : (part + 1) * cols]
                                    for i in (c, c | bit)
                                )
                            else:
                                a, b = (rim_packed[group, i, part] for i in (c, c | bit))
                            rim_packed[group, c, part] = jnp.where(low, a, pltpu.roll(b, bit, 1))
                            rim_packed[group, c | bit, part] = jnp.where(
                                low, pltpu.roll(a, tile - bit, 1), b
                            )
                bit *= 2

            @pl.loop(0, cols)
            def _(c):
                line = [rim_packed[group, c, part] for part in range(n_parts)]
                bit = 1
                while bit < n_parts:
                    high = ((lane_index // cols) & bit) != 0
                    line = [
                        jnp.where(high, line[(part + bit) % n_parts], line[part])
                        for part in range(n_parts)
                    ]
                    bit *= 2
                for part in range(n_parts):
                    rim_packed[group, c, part] = line[part]

    def turn(block, shift):
        return pltpu.roll(block, shift % tile, 1) if shift % tile else block

    def rim_line(group, rows_in, sums):
        for part in range(n_parts):
            total = rim_packed[group, 0, part] * rows_in[0]
            for c in range(1, cols):
                total = total + rim_packed[group, c, part] * rows_in[c]
            sums = sums + [turn(total, part * cols)]
        while len(sums) > 1:
            sums = [sum(sums[i + 1 : i + 2], sums[i]) for i in range(0, len(sums), 2)]
        return sums[0]

    def crossing(lines, total):
        for r, block in lines:
            total = jnp.where(within == rows + r, turn(block, rows + r), total)
            total = jnp.where(within == r, turn(block, r + 1 - cols), total)
        return total

    middle = range(1, rows - 1)
    outer = [0, rows - 1]
    nothing = jnp.zeros((cols, tile), jnp.float32)

    def finish(k, last):
        parts = [repack(fields[k + 1, r]) for r in range(rows)]
        receive(k, (LEFT, RIGHT))
        line = rim_line(
            2,
            [
                jnp.where(within < rows, halo_cols[k, 0, c : c + 1], halo_cols[k, 1, c : c + 1])
                for c in range(cols)
            ],
            [],
        )
        for r in range(rows):
            parts[r] = parts[r] + jnp.where(
                within == 0,
                turn(line, -r),
                jnp.where(within == cols - 1, turn(line, cols - 1 - rows - r), 0.0),
            )
        for r in middle:
            fields[k + 1, r] = repack(parts[r])
        if last:
            known = products(k, middle)
        else:
            known = crossing([(r, parts[r]) for r in middle], nothing)
        receive(k, (ABOVE, BELOW))
        for side, r in enumerate(outer):
            parts[r] = rim_line(
                side, [halo_rows[k, side, c : c + 1] for c in range(cols)], [parts[r]]
            )
            if not last:
                packed[k + 1, r] = parts[r]
        if not last:
            send(k + 1, (ABOVE, BELOW))
            cross[k + 1] = crossing([(r, parts[r]) for r in outer], known)
            send(k + 1, (LEFT, RIGHT))
        for r in outer:
            fields[k + 1, r] = repack(parts[r])
        if last:
            late[...] = line_of(known + products(k, outer), 0)

    def edges():
        for r in range(rows):
            edge_cols[0, r : r + 1] = fields[0, r, 0:1]
            edge_cols[1, r : r + 1] = fields[0, r, cols - 1 : cols]

    pairs = prev + basis
    per_line = tile // pitch
    pair_lane = lax.broadcasted_iota(jnp.int32, (pairs, tile), 1)
    pair_index = lax.broadcasted_iota(jnp.int32, (pairs, tile), 0)
    line_index = lax.broadcasted_iota(jnp.int32, stats.shape, 0)

    def products(k, lines):
        values = []
        for g in range(groups_prev + 1):
            total = None
            for r in lines:
                if g < groups_prev:
                    other = earlier[g * basis : (g + 1) * basis, r]
                else:
                    other = fields[1 : basis + 1, r]
                term = other * fields[k + 1, r][None]
                total = term if total is None else total + term
            values.append(jnp.sum(total, axis=1))
        return jnp.concatenate(values, axis=0)

    def inner(k):
        record(k, products(k, range(rows)))

    def line_of(values, start):
        value = jnp.sum(values, axis=1, keepdims=True)
        return jnp.sum(
            jnp.where(pair_lane == start + pair_index, value, 0.0), axis=0, keepdims=True
        )

    def record(k, values):
        line = line_of(values, (k % per_line) * pitch)
        stats[...] += jnp.where(line_index == k // per_line, line, 0.0)

    small[0].wait()
    small[1].wait()
    for r in range(1, rows):
        for c in range(cols):
            load(r, c).start()
    start = weights_ref[0] * earlier[0]
    for p in range(1, prev):
        start = start + weights_ref[p] * earlier[p]
    fields[0] = start
    for r in (0, rows - 1):
        packed[0, r] = fields[0, r]
    edges()
    pl.semaphore_wait(barrier, peers - 1)
    send(0, range(4), True)
    for copy in small[2:]:
        copy.wait()
    for s, lines in enumerate(code_columns()):
        for r, line in enumerate(lines):
            code_table[s, r] = line
    inside(0, True)
    gather_rim()

    receive(0, range(4), True)
    rim()
    lines = [(r, repack(fields[1, r])) for r in range(rows)]
    for r in (0, rows - 1):
        packed[1, r] = lines[r][1]
    send(1, (ABOVE, BELOW))
    cross[1] = crossing(lines, nothing)
    send(1, (LEFT, RIGHT))
    inside(1, False)
    pack_rim()

    @pl.loop(1, basis - 1)
    def _(k):
        finish(k, False)
        inside(k + 1, False)

        @pl.when(k == 1)
        def _():
            inner(0)

        inner(k)

    def deliver(src, dst, send_sem, recv_sem):
        for other in others:
            pltpu.make_async_remote_copy(
                src_ref=src,
                dst_ref=dst.at[me],
                send_sem=send_sem,
                recv_sem=recv_sem,
                device_id=other,
                device_id_type=MESH,
            ).start()

    def collect(dst, sem):
        whole = dst.at[pl.ds(0, peers - 1)]
        pltpu.make_async_copy(whole, whole, sem).wait()

    deliver(stats, gathered, all_sem.at[0], all_sem.at[1])
    gathered[me] = stats[...]
    finish(basis - 1, True)

    deliver(late, late_gathered, all_sem.at[2], all_sem.at[3])

    def sent(k, first):
        for direction in range(4):
            @pl.when(has[direction])
            def _(direction=direction):
                hop(k, direction, first).wait_send()

    sent(0, True)

    @pl.loop(1, basis)
    def _(k):
        sent(k, False)

    late_gathered[me] = late[...]
    collect(gathered, all_sem.at[0])
    collect(gathered, all_sem.at[1])
    newest = basis - 1
    total = jnp.sum(gathered[...], axis=0) * (1.0 / cells)
    turned = total.T
    proj = [None] * pairs
    for k in range(newest):
        for g in range(groups_prev + 1):
            first = (k % per_line) * pitch + g * basis
            column = turned[first : first + basis, k // per_line : k // per_line + 1]
            column = jnp.broadcast_to(column, (basis, tile))
            spread[g * basis + k] = column
            proj[g * basis + k] = column
        first = (k % per_line) * pitch
        proj_ref[k : k + 1, :] = total[k // per_line : k // per_line + 1, first : first + prev]

    def clean(k):
        value = fields[k + 1]
        for p in range(prev):
            g, q = p // basis, p % basis
            value = value - spread[g * basis + k, q : q + 1][None] * earlier[p]
        return value

    def gram_of(j, k):
        removed = proj[j] * proj[k]
        for g in range(1, groups_prev):
            removed = removed + proj[g * basis + j] * proj[g * basis + k]
        return spread[groups_prev * basis + k, j : j + 1] - jnp.sum(
            removed, axis=0, keepdims=True
        )

    for k in range(newest):
        basis_ref[k] = clean(k)
    gram = {(j, k): gram_of(j, k) for j in range(newest) for k in range(j, newest)}
    lower, inverse = {}, []
    for j in range(newest):
        root = jnp.sqrt(gram[j, j])
        inverse.append(1.0 / root)
        lower[j, j] = root
        for k in range(j + 1, newest):
            lower[k, j] = gram[j, k] * inverse[j]
        for k in range(j + 1, newest):
            for m in range(k, newest):
                gram[k, m] = gram[k, m] - lower[k, j] * lower[m, j]

    for r in range(rows):
        done = []
        for k in range(newest):
            value = basis_ref[k, r]
            for j in range(k):
                value = value - lower[k, j] * done[j]
            value = value * inverse[k]
            done.append(value)
            basis_ref[k, r] = value

    collect(late_gathered, all_sem.at[2])
    collect(late_gathered, all_sem.at[3])
    last_line = jnp.sum(late_gathered[...], axis=0) * (1.0 / cells)
    turned = jnp.broadcast_to(last_line, (tile, tile)).T
    for g in range(groups_prev + 1):
        column = turned[g * basis : (g + 1) * basis]
        spread[g * basis + newest] = column
        proj[g * basis + newest] = column
    proj_ref[newest : newest + 1, :] = last_line[:, :prev]
    square = gram_of(newest, newest)
    for j in range(newest):
        value = gram_of(j, newest)
        for i in range(j):
            value = value - lower[j, i] * lower[newest, i]
        lower[newest, j] = value * inverse[j]
        square = square - lower[newest, j] * lower[newest, j]
    lower[newest, newest] = jnp.sqrt(square)
    value = clean(newest)
    for j in range(newest):
        value = value - lower[newest, j][None] * basis_ref[j]
    basis_ref[newest] = value * (1.0 / lower[newest, newest])[None]

    row_index = lax.broadcasted_iota(jnp.int32, (basis, tile), 0)
    upper = jnp.zeros((basis, tile), jnp.float32)
    for j in range(basis):
        line = jnp.zeros((1, tile), jnp.float32)
        for k in range(j, basis):
            line = jnp.where(lane[0:1] == k, lower[k, j], line)
        upper = jnp.where(row_index == j, line, upper)
    upper_ref[...] = upper[:, :basis]


def store(basis_ref, upper_ref, proj_ref, basis_hbm, upper_hbm, proj_hbm, sem):
    copies = [
        pltpu.make_async_copy(src, dst, sem.at[i])
        for i, (src, dst) in enumerate(
            [(basis_ref, basis_hbm), (upper_ref, upper_hbm), (proj_ref, proj_hbm)]
        )
    ]
    for copy in copies:
        copy.start()
    for copy in copies:
        copy.wait()


def shards(n_rows, n_cols, tile_blocks, tile_codes, shifts, shift_order, earlier, start_weights):
    rows, cols, slots, tile, _ = tile_blocks.shape
    basis, prev = shifts.shape[0], earlier.shape[0]
    peers = n_rows * n_cols
    pitch = pl.next_power_of_2(prev + basis)
    lines = pl.cdiv(basis, tile // pitch)
    vmem = pl.BlockSpec(memory_space=pltpu.VMEM)
    hbm = pl.BlockSpec(memory_space=pltpu.HBM)
    codes = jnp.transpose(tile_codes, (2, 0, 1))
    f32 = jnp.float32
    basis_out, upper, proj = pl.pallas_call(
        functools.partial(kernel, n_rows, n_cols, pitch),
        out_shape=(
            jax.ShapeDtypeStruct((basis, rows, cols, tile), f32),
            jax.ShapeDtypeStruct((basis, basis), f32),
            jax.ShapeDtypeStruct((basis, prev), f32),
        ),
        in_specs=[hbm] * 6,
        out_specs=(vmem, vmem, vmem),
        scratch_shapes=[
            pltpu.VMEM(tile_blocks.shape, f32),
            pltpu.VMEM(earlier.shape, f32),
            pltpu.VMEM(codes.shape, jnp.int32),
            pltpu.SMEM(shifts.shape, f32),
            pltpu.SMEM(shift_order.shape, jnp.int32),
            pltpu.SMEM(start_weights.shape, f32),
            pltpu.VMEM((basis + 1, rows, cols, tile), f32),
            pltpu.VMEM((slots, rows, cols, tile), f32),
            pltpu.VMEM((basis, rows, cols, tile), f32),
            pltpu.VMEM((basis, cols, tile), f32),
            pltpu.VMEM((3, cols, tile // cols, cols, tile), f32),
            pltpu.VMEM((basis, 2, cols, tile), f32),
            pltpu.VMEM((basis, 2, cols, tile), f32),
            pltpu.VMEM((2, rows, tile), f32),
            pltpu.VMEM((2, rows, tile), f32),
            pltpu.VMEM((3, cols, tile, tile), f32),
            pltpu.VMEM((slots - 1, rows, cols, tile), f32),
            pltpu.VMEM((lines, tile), f32),
            pltpu.VMEM((peers, lines, tile), f32),
            pltpu.VMEM((1, tile), f32),
            pltpu.VMEM((peers, 1, tile), f32),
            pltpu.VMEM(((prev // basis + 1) * basis, basis, tile), f32),
            pltpu.SemaphoreType.DMA((rows, cols)),
            pltpu.SemaphoreType.DMA((5,)),
            pltpu.SemaphoreType.DMA((basis, 4)),
            pltpu.SemaphoreType.DMA((basis, 4)),
            pltpu.SemaphoreType.DMA((4,)),
        ],
        compiler_params=pltpu.CompilerParams(
            collective_id=0, has_side_effects=True, vmem_limit_bytes=48 * 1024 * 1024
        ),
        name="sstep",
    )(*[pltpu.with_memory_space_constraint(x, pltpu.HBM) for x in (tile_blocks, codes, shifts, shift_order, earlier, start_weights)])
    results = (basis_out, upper, proj)
    basis_out, upper, proj = pl.pallas_call(
        store,
        out_shape=tuple(jax.ShapeDtypeStruct(x.shape, f32) for x in results),
        in_specs=[vmem] * 3,
        out_specs=(hbm,) * 3,
        scratch_shapes=[pltpu.SemaphoreType.DMA((3,))],
        name="store",
    )(*[pltpu.with_memory_space_constraint(x, pltpu.VMEM) for x in results])
    return basis_out, upper, proj.T


def solution(mesh):
    in_specs = (
        P(("groups", "rows"), "cols", None, None, None),
        P(("groups", "rows"), "cols", None),
        P("groups"),
        P("groups"),
        P(None, ("groups", "rows"), "cols", None),
        P("groups"),
    )
    out_specs = (P(None, ("groups", "rows"), "cols", None), P("groups", None), P("groups", None))
    body = functools.partial(shards, mesh.shape["rows"], mesh.shape["cols"])
    return jax.shard_map(body, mesh=mesh, in_specs=in_specs, out_specs=out_specs, check_vma=False)
```

```python
import functools

import jax
import jax.numpy as jnp
from jax import lax
from jax.experimental import pallas as pl
from jax.experimental.pallas import tpu as pltpu
from jax.sharding import PartitionSpec as P

MESH = pl.DeviceIdType.MESH
ABOVE, BELOW, LEFT, RIGHT = range(4)


def kernel(
    n_rows, n_cols, pitch,
    blocks_hbm, codes_hbm, shifts_hbm, order_hbm, earlier_hbm, weights_hbm,
    basis_ref, upper_ref, proj_ref,
    blocks, earlier, codes_ref, shifts_ref, order_ref, weights_ref,
    fields, chosen, packed, cross, rim_packed, halo_rows, halo_cols, first_cols, edge_cols, rim_tiles,
    code_table, stats, gathered, late, late_gathered, spread,
    load_sem, small_sem, send_sem, recv_sem, all_sem,
):
    rows, cols, slots, tile, _ = blocks.shape
    basis = basis_ref.shape[0]
    prev = earlier.shape[0]
    groups_prev = prev // basis
    peers = n_rows * n_cols
    cells = float(peers * rows * cols * tile)
    my_row, my_col = lax.axis_index("rows"), lax.axis_index("cols")
    me = my_row * n_cols + my_col

    def load(r, c):
        return pltpu.make_async_copy(
            blocks_hbm.at[r, c], blocks.at[r, c], load_sem.at[r, c]
        )

    small = [
        pltpu.make_async_copy(src, dst, small_sem.at[i])
        for i, (src, dst) in enumerate(
            [
                (weights_hbm, weights_ref),
                (earlier_hbm, earlier),
                (codes_hbm, codes_ref),
                (shifts_hbm, shifts_ref),
                (order_hbm, order_ref),
            ]
        )
    ]
    for copy in small:
        copy.start()

    barrier = pltpu.get_barrier_semaphore()
    all_rows = [lax.rem(my_row + d, n_rows) for d in range(n_rows)]
    all_cols = [lax.rem(my_col + d, n_cols) for d in range(n_cols)]
    others = [{"rows": r, "cols": c} for r in all_rows for c in all_cols][1:]
    others = others[n_cols - 1 :] + others[: n_cols - 1]
    for other in others:
        pl.semaphore_signal(barrier, inc=1, device_id=other, device_id_type=MESH)

    line_order = [0, rows - 1, *range(1, rows - 1)]
    for c in range(cols):
        load(line_order[0], c).start()

    for k in range(1, basis + 1):
        fields[k] = jnp.zeros((rows, cols, tile), jnp.float32)
    stats[...] = jnp.zeros_like(stats)
    no_row = jnp.zeros((basis, cols, tile), jnp.float32)
    no_first = jnp.zeros((rows, tile), jnp.float32)
    has = [my_row > 0, my_row < n_rows - 1, my_col > 0, my_col < n_cols - 1]

    @pl.when(my_row == 0)
    def _():
        halo_rows[:, 0] = no_row

    @pl.when(my_row == n_rows - 1)
    def _():
        halo_rows[:, 1] = no_row

    @pl.when(my_col == 0)
    def _():
        halo_cols[:, 0] = no_row
        first_cols[0] = no_first

    @pl.when(my_col == n_cols - 1)
    def _():
        halo_cols[:, 1] = no_row
        first_cols[1] = no_first

    def hop(k, direction, first=False):
        if direction == ABOVE:
            src, dst, where_to = packed.at[k, 0], halo_rows.at[k, 1], {"rows": my_row - 1}
        elif direction == BELOW:
            src, dst, where_to = packed.at[k, rows - 1], halo_rows.at[k, 0], {"rows": my_row + 1}
        else:
            side = direction - LEFT
            where_to = {"cols": my_col + 2 * side - 1}
            if first:
                src, dst = edge_cols.at[side], first_cols.at[1 - side]
            else:
                src, dst = cross.at[k], halo_cols.at[k, 1 - side]
        return pltpu.make_async_remote_copy(
            src_ref=src,
            dst_ref=dst,
            send_sem=send_sem.at[k, direction],
            recv_sem=recv_sem.at[k, direction ^ 1],
            device_id=where_to,
            device_id_type=MESH,
        )

    def arrival(k, direction, first):
        if direction in (ABOVE, BELOW):
            dst = halo_rows.at[k, direction]
        elif first:
            dst = first_cols.at[direction - LEFT]
        else:
            dst = halo_cols.at[k, direction - LEFT]
        return pltpu.make_async_copy(dst, dst, recv_sem.at[k, direction])

    def send(k, directions, first=False):
        for direction in directions:
            @pl.when(has[direction])
            def _(direction=direction):
                hop(k, direction, first).start()

    def receive(k, directions, first=False):
        for direction in directions:
            @pl.when(has[direction])
            def _(direction=direction):
                arrival(k, direction, first).wait()

    sublane = lax.broadcasted_iota(jnp.int32, (cols, tile), 0)
    lane = lax.broadcasted_iota(jnp.int32, (basis, tile), 1)
    diagonal = lax.broadcasted_iota(jnp.int32, (cols, cols), 0) == lax.broadcasted_iota(
        jnp.int32, (cols, cols), 1
    )

    lane_index = lax.broadcasted_iota(jnp.int32, (cols, tile), 1)
    within = lane_index % cols
    offset = within - sublane
    n_parts = tile // cols

    def code_columns():
        codes = codes_ref[...].astype(jnp.float32)
        masks = []
        for s in range(slots - 1):
            masks.append([])
            for r in range(rows):
                line = jnp.broadcast_to(codes[s, r : r + 1], (cols, cols))
                column = jnp.sum(jnp.where(diagonal, line, 0.0), axis=1, keepdims=True)
                masks[s].append(jnp.broadcast_to(column, (cols, tile)))
        return masks

    def choose(k):
        none = jnp.zeros((cols, tile), jnp.float32)
        for r in range(rows):
            here = fields[k, r]
            above = fields[k, r - 1] if r > 0 else none
            below = fields[k, r + 1] if r < rows - 1 else none
            left = jnp.where(sublane == 0, 0.0, pltpu.roll(here, 1, 0))
            right = jnp.where(sublane == cols - 1, 0.0, pltpu.roll(here, cols - 1, 0))
            chosen[0, r] = here
            for s in range(slots - 1):
                code = code_table[s, r]
                chosen[s + 1, r] = jnp.where(
                    code < 1.5,
                    jnp.where(code < 0.5, above, below),
                    jnp.where(code < 2.5, left, right),
                )

    def line_inside(k, r, shift):
        for c in range(cols):
            total = blocks[r, c, 0] * chosen[0, r, c : c + 1]
            for s in range(1, slots):
                total = total + blocks[r, c, s] * chosen[s, r, c : c + 1]
            product = jnp.sum(total.T, axis=0, keepdims=True)
            fields[k + 1, r, c : c + 1] = product - shift * chosen[0, r, c : c + 1]

    def inside(k):
        shift = shifts_ref[order_ref[k]]
        choose(k)

        @pl.loop(0, rows)
        def _(r):
            line_inside(k, r, shift)

    def inside_first():
        shift = shifts_ref[order_ref[0]]
        choose(0)
        for r in line_order:
            for c in range(cols):
                load(r, c).wait()
            line_inside(0, r, shift)
            for side in range(2):
                if r == side * (rows - 1):
                    gather_line(side)
                rim_tiles[2, side * rows + r] = pick(r, side * (cols - 1), side + LEFT)

    def pick(r, c, direction):
        total = jnp.zeros((tile, tile), jnp.float32)
        for s in range(slots - 1):
            code = code_table[s, r, c : c + 1]
            total = jnp.where(code == float(direction), blocks[r, c, s + 1], total)
        return total

    def gather_line(side):
        @pl.loop(0, cols)
        def _(c):
            total = jnp.zeros((tile, tile), jnp.float32)
            for s in range(slots - 1):
                code = code_table[s, side * (rows - 1), pl.ds(c, 1)]
                total = jnp.where(
                    code == float(side), blocks[side * (rows - 1), c, s + 1], total
                )
            rim_tiles[side, c] = total

    def rim():
        for r in range(rows):
            for c in range(cols):
                parts = []
                for side in range(2):
                    if r == side * (rows - 1):
                        parts.append(rim_tiles[side, c] * halo_rows[0, side, c : c + 1])
                    if c == side * (cols - 1):
                        parts.append(
                            rim_tiles[2, side * rows + r] * first_cols[side, r : r + 1]
                        )
                if parts:
                    product = jnp.sum(sum(parts[1:], parts[0]).T, axis=0, keepdims=True)
                    fields[1, r, c : c + 1] += product

    def repack(block):
        total = jnp.where(offset == 0, block, 0.0)
        for shift in range(1, cols):
            turned = pltpu.roll(block, cols - shift, 0)
            total = jnp.where(offset == shift, pltpu.roll(turned, shift, 1), total)
            total = jnp.where(
                offset == shift - cols, pltpu.roll(turned, tile + shift - cols, 1), total
            )
        return total

    def pack_rim():
        @pl.loop(0, 3)
        def _(group):
            bit = 1
            while bit < cols:
                low = (lane_index & bit) == 0
                for part in range(n_parts):
                    for c in range(cols):
                        if c & bit == 0:
                            if bit == 1:
                                a, b = (
                                    rim_tiles[group, i, part * cols : (part + 1) * cols]
                                    for i in (c, c | bit)
                                )
                            else:
                                a, b = (rim_packed[group, i, part] for i in (c, c | bit))
                            rim_packed[group, c, part] = jnp.where(low, a, pltpu.roll(b, bit, 1))
                            rim_packed[group, c | bit, part] = jnp.where(
                                low, pltpu.roll(a, tile - bit, 1), b
                            )
                bit *= 2

            @pl.loop(0, cols)
            def _(c):
                line = [rim_packed[group, c, part] for part in range(n_parts)]
                bit = 1
                while bit < n_parts:
                    high = ((lane_index // cols) & bit) != 0
                    line = [
                        jnp.where(high, line[(part + bit) % n_parts], line[part])
                        for part in range(n_parts)
                    ]
                    bit *= 2
                for part in range(n_parts):
                    rim_packed[group, c, part] = line[part]

    def turn(block, shift):
        return pltpu.roll(block, shift % tile, 1) if shift % tile else block

    def rim_line(group, rows_in, sums):
        for part in range(n_parts):
            total = rim_packed[group, 0, part] * rows_in[0]
            for c in range(1, cols):
                total = total + rim_packed[group, c, part] * rows_in[c]
            sums = sums + [turn(total, part * cols)]
        while len(sums) > 1:
            sums = [sum(sums[i + 1 : i + 2], sums[i]) for i in range(0, len(sums), 2)]
        return sums[0]

    def crossing(lines, total):
        for r, block in lines:
            total = jnp.where(within == rows + r, turn(block, rows + r), total)
            total = jnp.where(within == r, turn(block, r + 1 - cols), total)
        return total

    middle = range(1, rows - 1)
    outer = [0, rows - 1]
    nothing = jnp.zeros((cols, tile), jnp.float32)

    def finish(k, last):
        parts = [repack(fields[k + 1, r]) for r in range(rows)]
        receive(k, (LEFT, RIGHT))
        line = rim_line(
            2,
            [
                jnp.where(within < rows, halo_cols[k, 0, c : c + 1], halo_cols[k, 1, c : c + 1])
                for c in range(cols)
            ],
            [],
        )
        for r in range(rows):
            parts[r] = parts[r] + jnp.where(
                within == 0,
                turn(line, -r),
                jnp.where(within == cols - 1, turn(line, cols - 1 - rows - r), 0.0),
            )
        for r in middle:
            fields[k + 1, r] = repack(parts[r])
        if last:
            known = products(k, middle)
        else:
            known = crossing([(r, parts[r]) for r in middle], nothing)
        receive(k, (ABOVE, BELOW))
        for side, r in enumerate(outer):
            parts[r] = rim_line(
                side, [halo_rows[k, side, c : c + 1] for c in range(cols)], [parts[r]]
            )
            if not last:
                packed[k + 1, r] = parts[r]
        if not last:
            send(k + 1, (ABOVE, BELOW))
            cross[k + 1] = crossing([(r, parts[r]) for r in outer], known)
            send(k + 1, (LEFT, RIGHT))
        for r in outer:
            fields[k + 1, r] = repack(parts[r])
        if last:
            late[...] = line_of(known + products(k, outer), 0)

    def edges():
        for r in range(rows):
            edge_cols[0, r : r + 1] = fields[0, r, 0:1]
            edge_cols[1, r : r + 1] = fields[0, r, cols - 1 : cols]

    pairs = prev + basis
    per_line = tile // pitch
    pair_lane = lax.broadcasted_iota(jnp.int32, (pairs, tile), 1)
    pair_index = lax.broadcasted_iota(jnp.int32, (pairs, tile), 0)
    line_index = lax.broadcasted_iota(jnp.int32, stats.shape, 0)

    def products(k, lines):
        values = []
        for g in range(groups_prev + 1):
            total = None
            for r in lines:
                if g < groups_prev:
                    other = earlier[g * basis : (g + 1) * basis, r]
                else:
                    other = fields[1 : basis + 1, r]
                term = other * fields[k + 1, r][None]
                total = term if total is None else total + term
            values.append(jnp.sum(total, axis=1))
        return jnp.concatenate(values, axis=0)

    def inner(k):
        record(k, products(k, range(rows)))

    def line_of(values, start):
        value = jnp.sum(values, axis=1, keepdims=True)
        return jnp.sum(
            jnp.where(pair_lane == start + pair_index, value, 0.0), axis=0, keepdims=True
        )

    def record(k, values):
        line = line_of(values, (k % per_line) * pitch)
        stats[...] += jnp.where(line_index == k // per_line, line, 0.0)

    small[0].wait()
    small[1].wait()
    for r in line_order[1:]:
        for c in range(cols):
            load(r, c).start()
    start = weights_ref[0] * earlier[0]
    for p in range(1, prev):
        start = start + weights_ref[p] * earlier[p]
    fields[0] = start
    for r in (0, rows - 1):
        packed[0, r] = fields[0, r]
    edges()
    pl.semaphore_wait(barrier, peers - 1)
    send(0, range(4), True)
    for copy in small[2:]:
        copy.wait()
    for s, lines in enumerate(code_columns()):
        for r, line in enumerate(lines):
            code_table[s, r] = line
    inside_first()

    receive(0, range(4), True)
    rim()
    lines = [(r, repack(fields[1, r])) for r in range(rows)]
    for r in (0, rows - 1):
        packed[1, r] = lines[r][1]
    send(1, (ABOVE, BELOW))
    cross[1] = crossing(lines, nothing)
    send(1, (LEFT, RIGHT))
    inside(1)
    pack_rim()

    for k in range(1, basis - 1):
        finish(k, False)
        inside(k + 1)
        if k == 1:
            inner(0)
        inner(k)

    def deliver(src, dst, send_sem, recv_sem):
        for other in others:
            pltpu.make_async_remote_copy(
                src_ref=src,
                dst_ref=dst.at[me],
                send_sem=send_sem,
                recv_sem=recv_sem,
                device_id=other,
                device_id_type=MESH,
            ).start()

    def collect(dst, sem):
        whole = dst.at[pl.ds(0, peers - 1)]
        pltpu.make_async_copy(whole, whole, sem).wait()

    deliver(stats, gathered, all_sem.at[0], all_sem.at[1])
    gathered[me] = stats[...]
    finish(basis - 1, True)

    deliver(late, late_gathered, all_sem.at[2], all_sem.at[3])

    def sent(k, first):
        for direction in range(4):
            @pl.when(has[direction])
            def _(direction=direction):
                hop(k, direction, first).wait_send()

    sent(0, True)

    @pl.loop(1, basis)
    def _(k):
        sent(k, False)

    late_gathered[me] = late[...]
    collect(gathered, all_sem.at[0])
    collect(gathered, all_sem.at[1])
    newest = basis - 1
    total = jnp.sum(gathered[...], axis=0) * (1.0 / cells)
    turned = total.T
    proj = [None] * pairs
    for k in range(newest):
        for g in range(groups_prev + 1):
            first = (k % per_line) * pitch + g * basis
            column = turned[first : first + basis, k // per_line : k // per_line + 1]
            column = jnp.broadcast_to(column, (basis, tile))
            spread[g * basis + k] = column
            proj[g * basis + k] = column
        first = (k % per_line) * pitch
        proj_ref[k : k + 1, :] = total[k // per_line : k // per_line + 1, first : first + prev]

    def clean(k):
        value = fields[k + 1]
        for p in range(prev):
            g, q = p // basis, p % basis
            value = value - spread[g * basis + k, q : q + 1][None] * earlier[p]
        return value

    def gram_of(j, k):
        removed = proj[j] * proj[k]
        for g in range(1, groups_prev):
            removed = removed + proj[g * basis + j] * proj[g * basis + k]
        return spread[groups_prev * basis + k, j : j + 1] - jnp.sum(
            removed, axis=0, keepdims=True
        )

    for k in range(newest):
        basis_ref[k] = clean(k)
    gram = {(j, k): gram_of(j, k) for j in range(newest) for k in range(j, newest)}
    lower, inverse = {}, []
    for j in range(newest):
        root = jnp.sqrt(gram[j, j])
        inverse.append(1.0 / root)
        lower[j, j] = root
        for k in range(j + 1, newest):
            lower[k, j] = gram[j, k] * inverse[j]
        for k in range(j + 1, newest):
            for m in range(k, newest):
                gram[k, m] = gram[k, m] - lower[k, j] * lower[m, j]

    for r in range(rows):
        done = []
        for k in range(newest):
            value = basis_ref[k, r]
            for j in range(k):
                value = value - lower[k, j] * done[j]
            value = value * inverse[k]
            done.append(value)
            basis_ref[k, r] = value

    collect(late_gathered, all_sem.at[2])
    collect(late_gathered, all_sem.at[3])
    last_line = jnp.sum(late_gathered[...], axis=0) * (1.0 / cells)
    turned = jnp.broadcast_to(last_line, (tile, tile)).T
    for g in range(groups_prev + 1):
        column = turned[g * basis : (g + 1) * basis]
        spread[g * basis + newest] = column
        proj[g * basis + newest] = column
    proj_ref[newest : newest + 1, :] = last_line[:, :prev]
    square = gram_of(newest, newest)
    for j in range(newest):
        value = gram_of(j, newest)
        for i in range(j):
            value = value - lower[j, i] * lower[newest, i]
        lower[newest, j] = value * inverse[j]
        square = square - lower[newest, j] * lower[newest, j]
    lower[newest, newest] = jnp.sqrt(square)
    value = clean(newest)
    for j in range(newest):
        value = value - lower[newest, j][None] * basis_ref[j]
    basis_ref[newest] = value * (1.0 / lower[newest, newest])[None]

    row_index = lax.broadcasted_iota(jnp.int32, (basis, tile), 0)
    upper = jnp.zeros((basis, tile), jnp.float32)
    for j in range(basis):
        line = jnp.zeros((1, tile), jnp.float32)
        for k in range(j, basis):
            line = jnp.where(lane[0:1] == k, lower[k, j], line)
        upper = jnp.where(row_index == j, line, upper)
    upper_ref[...] = upper[:, :basis]


def store(basis_ref, upper_ref, proj_ref, basis_hbm, upper_hbm, proj_hbm, sem):
    copies = [
        pltpu.make_async_copy(src, dst, sem.at[i])
        for i, (src, dst) in enumerate(
            [(basis_ref, basis_hbm), (upper_ref, upper_hbm), (proj_ref, proj_hbm)]
        )
    ]
    for copy in copies:
        copy.start()
    for copy in copies:
        copy.wait()


def shards(n_rows, n_cols, tile_blocks, tile_codes, shifts, shift_order, earlier, start_weights):
    rows, cols, slots, tile, _ = tile_blocks.shape
    basis, prev = shifts.shape[0], earlier.shape[0]
    peers = n_rows * n_cols
    pitch = pl.next_power_of_2(prev + basis)
    lines = pl.cdiv(basis, tile // pitch)
    vmem = pl.BlockSpec(memory_space=pltpu.VMEM)
    hbm = pl.BlockSpec(memory_space=pltpu.HBM)
    codes = jnp.transpose(tile_codes, (2, 0, 1))
    f32 = jnp.float32
    basis_out, upper, proj = pl.pallas_call(
        functools.partial(kernel, n_rows, n_cols, pitch),
        out_shape=(
            jax.ShapeDtypeStruct((basis, rows, cols, tile), f32),
            jax.ShapeDtypeStruct((basis, basis), f32),
            jax.ShapeDtypeStruct((basis, prev), f32),
        ),
        in_specs=[hbm] * 6,
        out_specs=(vmem, vmem, vmem),
        scratch_shapes=[
            pltpu.VMEM(tile_blocks.shape, f32),
            pltpu.VMEM(earlier.shape, f32),
            pltpu.VMEM(codes.shape, jnp.int32),
            pltpu.SMEM(shifts.shape, f32),
            pltpu.SMEM(shift_order.shape, jnp.int32),
            pltpu.SMEM(start_weights.shape, f32),
            pltpu.VMEM((basis + 1, rows, cols, tile), f32),
            pltpu.VMEM((slots, rows, cols, tile), f32),
            pltpu.VMEM((basis, rows, cols, tile), f32),
            pltpu.VMEM((basis, cols, tile), f32),
            pltpu.VMEM((3, cols, tile // cols, cols, tile), f32),
            pltpu.VMEM((basis, 2, cols, tile), f32),
            pltpu.VMEM((basis, 2, cols, tile), f32),
            pltpu.VMEM((2, rows, tile), f32),
            pltpu.VMEM((2, rows, tile), f32),
            pltpu.VMEM((3, cols, tile, tile), f32),
            pltpu.VMEM((slots - 1, rows, cols, tile), f32),
            pltpu.VMEM((lines, tile), f32),
            pltpu.VMEM((peers, lines, tile), f32),
            pltpu.VMEM((1, tile), f32),
            pltpu.VMEM((peers, 1, tile), f32),
            pltpu.VMEM(((prev // basis + 1) * basis, basis, tile), f32),
            pltpu.SemaphoreType.DMA((rows, cols)),
            pltpu.SemaphoreType.DMA((5,)),
            pltpu.SemaphoreType.DMA((basis, 4)),
            pltpu.SemaphoreType.DMA((basis, 4)),
            pltpu.SemaphoreType.DMA((4,)),
        ],
        compiler_params=pltpu.CompilerParams(
            collective_id=0, has_side_effects=True, vmem_limit_bytes=48 * 1024 * 1024
        ),
        name="sstep",
    )(*[pltpu.with_memory_space_constraint(x, pltpu.HBM) for x in (tile_blocks, codes, shifts, shift_order, earlier, start_weights)])
    results = (basis_out, upper, proj)
    basis_out, upper, proj = pl.pallas_call(
        store,
        out_shape=tuple(jax.ShapeDtypeStruct(x.shape, f32) for x in results),
        in_specs=[vmem] * 3,
        out_specs=(hbm,) * 3,
        scratch_shapes=[pltpu.SemaphoreType.DMA((3,))],
        name="store",
    )(*[pltpu.with_memory_space_constraint(x, pltpu.VMEM) for x in results])
    return basis_out, upper, proj.T


def solution(mesh):
    in_specs = (
        P(("groups", "rows"), "cols", None, None, None),
        P(("groups", "rows"), "cols", None),
        P("groups"),
        P("groups"),
        P(None, ("groups", "rows"), "cols", None),
        P("groups"),
    )
    out_specs = (P(None, ("groups", "rows"), "cols", None), P("groups", None), P("groups", None))
    body = functools.partial(shards, mesh.shape["rows"], mesh.shape["cols"])
    return jax.shard_map(body, mesh=mesh, in_specs=in_specs, out_specs=out_specs, check_vma=False)
```
